256 devices in a mesh: tok: 8 (over z), tile: 16 (over y, x_lo, core), pair: 2 (over x_hi).
Axes of the slice: x: 4 (x_hi: 2, x_lo: 2; x = x_hi * 2 + x_lo), y: 4, z: 8, core: 2. Of those that a mesh axis runs over, the one named last changes fastest.
Arguments:
- inputs: bfloat16 [8192, 4096], P(('tok', 'pair'), 'tile'), may hold values from -6 to 6
- output_grads: bfloat16 [8192, 4096], P(('tok', 'pair'), 'tile'), may hold values from -0.0625 to 0.0625
- statistics: float32 [16, 2, 1024, 1024], P('tile', 'pair', 'tok'), may hold values from -30 to 43008, as said below
Outputs:
- update: bfloat16 [16, 1024, 1024], P('tile', ('tok', 'pair'))
- new_statistics: float32 [16, 2, 1024, 1024], P('tile', 'pair', 'tok')
The draws below stay inside these ranges and needn't reach their ends.
Inputs may be any that keep to these rules, and one draw needn't show every extreme that they name: `statistics`: for every block and factor the 1024 x 1024 matrix is symmetric and positive definite.
All inputs are finite; a program needn't handle non-finite values. Where the reference program divides by a largest or mean magnitude, that divisor is 1e-20 or more.
Results may differ from the reference program's by a relative error of at most 0.00325.
The reference program's roundings to bfloat16 on the way count: a program that leaves them out, or rounds other values in their place, can miss the bound.
Values may be sent and summed in bfloat16 or wider, within the bound.
No kernel may reach another device: no remote copies, remote signals or barrier semaphores. Data moves between devices by JAX's collectives and lax.ppermute only.
A program may use at most 64 MiB of HBM per device.

```python
import jax
import jax.numpy as jnp
from jax import lax

D = 4096
O = 1024
ITERS = 2
NB = 16
TOKENS = 8192


def draw_statistics(key, part):
    base_key = jax.random.fold_in(key, 7)
    noise_key, extra_key, scale_key = jax.random.split(base_key, 3)
    noise_draw = jnp.clip(jax.random.normal(noise_key, (NB, 2, O, O), jnp.float32), -1.7, 1.7)
    log_range = jnp.log(10.0)
    symmetric = (noise_draw + jnp.swapaxes(noise_draw, 2, 3)) * 0.7071
    identity = jnp.eye(O, dtype=jnp.float32)
    off_part = symmetric * (1.0 - identity)
    spread = jnp.sum(jnp.abs(off_part), axis=3)
    extra_diag = jax.random.uniform(extra_key, (NB, 2, O), jnp.float32, 0.25 * O, 0.5 * O)
    diagonal = 1.25 * spread + extra_diag
    matrix = off_part + diagonal[..., None] * identity
    scales = jnp.exp(jax.random.uniform(scale_key, (NB, 2, O), jnp.float32, 0.0, 1.0) * log_range)
    root_scales = jnp.sqrt(scales)
    return 0.1 * root_scales[..., :, None] * matrix * root_scales[..., None, :]


def shard_levels(stream_key, shape, cuts, least, high):
    def one(position, blocks):
        heights = jax.random.uniform(jax.random.fold_in(jax.random.fold_in(stream_key, 6), position), (blocks,), jnp.float32, least / len(cuts), high / len(cuts))
        return jnp.repeat(jnp.exp(heights), shape[position] // blocks).reshape((-1,) + (1,) * (len(shape) - position - 1))

    factor_of = one(*cuts[0])
    for cut in cuts[1:]:
        factor_of = factor_of * one(*cut)
    return factor_of


def gaussian(rng, extent, scale, most, pieces=(), kind=jnp.bfloat16):
    array = scale * jax.random.normal(rng, extent, jnp.float32)
    if pieces:
        array = array * shard_levels(rng, extent, pieces, -0.22, 0.18)
    return jnp.clip(array, -most, most).astype(kind)


def setup_inputs(seed: int = 0) -> dict:
    arg_keys = jax.random.split(jax.random.key(seed), 4)
    return {
        "inputs": gaussian(arg_keys[0], (TOKENS, D), 1.0, 6.0, ((0, 16), (1, 16))),
        "output_grads": gaussian(arg_keys[1], (TOKENS, D), TOKENS ** -0.5, 0.0625, ((0, 16), (1, 16))),
        "statistics": draw_statistics(jax.random.fold_in(arg_keys[3], 71), 0),
    }


def inverse_root(updated):
    identity = jnp.eye(O, dtype=jnp.float32)
    bound_max = jnp.max(lax.optimization_barrier(jnp.sum(jnp.abs(updated), axis=1)))
    iterate = ((updated + 0.1 * bound_max * identity) / (1.1 * bound_max)).astype(jnp.bfloat16)
    iterate = lax.optimization_barrier(iterate)
    root_whole = iterate
    for iteration in range(ITERS):
        factor = ((5.0 * identity - iterate.astype(jnp.float32)) / 4.0).astype(jnp.bfloat16)
        if iteration == 0:
            root_whole = factor
        else:
            root_whole = jnp.dot(root_whole, factor, preferred_element_type=jnp.float32).astype(jnp.bfloat16)
        if iteration + 1 < ITERS:
            square = jnp.dot(factor, factor, preferred_element_type=jnp.float32).astype(jnp.bfloat16)
            fourth = jnp.dot(square, square, preferred_element_type=jnp.float32).astype(jnp.bfloat16)
            iterate = jnp.dot(fourth, iterate, preferred_element_type=jnp.float32).astype(jnp.bfloat16)
            iterate = lax.optimization_barrier(iterate)
    return root_whole

def reference(inputs, output_grads, statistics):
    per_side = D // O

    def block_step(operands):
        block_index, previous = operands
        row_start = (block_index // per_side * O).astype(jnp.int32)
        col_start = (block_index % per_side * O).astype(jnp.int32)
        left_acts = lax.dynamic_slice_in_dim(inputs, row_start, O, 1)
        right_cots = lax.dynamic_slice_in_dim(output_grads, col_start, O, 1)
        gradient = jnp.dot(left_acts.T, right_cots, preferred_element_type=jnp.float32)
        grad_bf = gradient.astype(jnp.bfloat16)
        grad_sq = jnp.sum(jnp.square(grad_bf.astype(jnp.float32)))
        left_stat = 0.9 * previous[0] + 0.1 * jnp.dot(grad_bf, grad_bf.T, preferred_element_type=jnp.float32)
        right_stat = 0.9 * previous[1] + 0.1 * jnp.dot(grad_bf.T, grad_bf, preferred_element_type=jnp.float32)
        left_root = inverse_root(left_stat)
        right_root = inverse_root(right_stat)
        left_mixed = jnp.dot(left_root, grad_bf, preferred_element_type=jnp.float32).astype(jnp.bfloat16)
        raw_update = jnp.dot(left_mixed, right_root, preferred_element_type=jnp.float32)
        update_sq = jnp.sum(raw_update * raw_update)
        updated_block = (raw_update * jnp.sqrt(grad_sq / (update_sq + 1e-06))).astype(jnp.bfloat16)
        return (updated_block, jnp.stack([left_stat, right_stat]))
    updates, new_statistics = lax.map(block_step, (jnp.arange(NB, dtype=jnp.int32), statistics))
    return (updates, new_statistics)
```

```python
import jax
import jax.numpy as jnp
from jax import lax
from jax.experimental import pallas as pl
from jax.experimental.pallas import tpu as pltpu
from jax.sharding import Mesh, PartitionSpec as P


F32 = jnp.float32
BF16 = jnp.bfloat16
F16 = jnp.float16
VMEM = pl.BlockSpec(memory_space=pltpu.VMEM)
SMEM = pl.BlockSpec(memory_space=pltpu.SMEM)
Z = 8
LIMIT = 56 * 1024 * 1024


def params():
    return pltpu.CompilerParams(vmem_limit_bytes=LIMIT)


def dot(a, b, ca=1, cb=0):
    return lax.dot_general(a, b, (((ca,), (cb,)), ((), ())), preferred_element_type=F32)


def shift(x, axis, size, d):
    return lax.ppermute(x, axis, [(i, (i + d) % size) for i in range(size)])


def flip(x, axis, size, d):
    return lax.ppermute(x, axis, [(i, i ^ d) for i in range(size)])


def partial_kernel(idx, *refs):
    a_own, a_oth, b = refs[:4], refs[4:8], refs[8:12]
    out, peak, a_s, b_s = refs[12:]
    pair, xl, co, y = idx[0], idx[1], idx[2], idx[3]
    for d in range(4):
        p, l = pair ^ (d & 1), xl ^ (d >> 1)
        a_s[p, l * 2 + co] = a_own[d][...]
        a_s[p, l * 2 + 1 - co] = a_oth[d][...]
        src = y ^ d
        b_s[src & 1, src >> 1] = b[d][...]
    top = None
    for ca in range(4):
        for cb in range(2):
            acc = dot(a_s[0, ca], b_s[0, cb], 0, 0) + dot(a_s[1, ca], b_s[1, cb], 0, 0)
            out[256 * ca:256 * (ca + 1), 256 * cb:256 * (cb + 1)] = acc
            m = jnp.max(jnp.abs(acc), axis=0, keepdims=True)
            top = m if top is None else jnp.maximum(top, m)
    peak[...] = jnp.broadcast_to(jnp.max(top), peak.shape)


def stats_kernel(idx, *refs):
    g_own, g_oth, st = refs[:8], refs[8:16], refs[16:24]
    g_out, it_out, rows_out, sq_out, s_s = refs[24:]
    z, co = idx[0], idx[1]

    def place(own_col):
        oth_col = 1 - own_col
        for d in range(Z):
            r = pl.multiple_of(((z + Z - d) % Z) * 128, 128)
            for cb in range(2):
                c0 = (2 * cb + own_col) * 256
                c1 = (2 * cb + oth_col) * 256
                g_out[pl.ds(r, 128), c0:c0 + 256] = g_own[d][:, 256 * cb:256 * cb + 256]
                g_out[pl.ds(r, 128), c1:c1 + 256] = g_oth[d][:, 256 * cb:256 * cb + 256]

    pl.when(co == 0)(lambda: place(0))
    pl.when(co == 1)(lambda: place(1))
    for d in range(Z):
        rb = (z + Z - d) % Z
        r = pl.multiple_of(rb * 128, 128)
        for k in range(5):
            cb = (rb + k) % Z
            c = pl.multiple_of(cb * 128, 128)
            blk = 0.9 * st[d][:, 128 * k:128 * (k + 1)]
            s_s[cb, pl.ds(r, 128)] = blk
            if 0 < k < 4:
                s_s[rb, pl.ds(c, 128)] = blk.T

    def product(left):
        for j in range(4):
            if left:
                p = dot(g_out[...], g_out[256 * j:256 * (j + 1), :], 1, 1)
            else:
                p = dot(g_out[...], g_out[:, 256 * j:256 * (j + 1)], 0, 0)
            s_s[2 * j] = s_s[2 * j] + 0.1 * p[:, :128]
            s_s[2 * j + 1] = s_s[2 * j + 1] + 0.1 * p[:, 128:]

    pl.when(co == 0)(lambda: product(True))
    pl.when(co == 1)(lambda: product(False))
    top = None
    for j in range(Z):
        m = jnp.sum(jnp.abs(s_s[j]), axis=0, keepdims=True)
        top = m if top is None else jnp.maximum(top, m)
    bound = jnp.max(top, axis=1, keepdims=True)
    inv = 1.0 / (1.1 * bound)
    eye = (lax.broadcasted_iota(jnp.int32, (128, 128), 0)
           == lax.broadcasted_iota(jnp.int32, (128, 128), 1)).astype(F32)
    ridge = (0.1 * bound) * eye
    zr = pl.multiple_of(z * 128, 128)
    for j in range(Z):
        rows_out[:, 128 * j:128 * (j + 1)] = s_s[j, pl.ds(zr, 128)]
        it_out[:, 128 * j:128 * (j + 1)] = (s_s[j] * inv).astype(BF16)
        lo = 128 * j
        it_out[lo:lo + 128, lo:lo + 128] = ((s_s[j, lo:lo + 128] + ridge) * inv).astype(BF16)
    acc = None
    for j in range(8):
        v = g_out[128 * j:128 * (j + 1), :].astype(F32)
        s = jnp.sum(v * v, axis=0, keepdims=True)
        acc = s if acc is None else acc + s
    sq_out[...] = jnp.broadcast_to(jnp.sum(acc), sq_out.shape)


def negate_quarter(dst, src):
    eye = (lax.broadcasted_iota(jnp.int32, (256, 256), 0)
           == lax.broadcasted_iota(jnp.int32, (256, 256), 1)).astype(F32)
    for j in range(4):
        c = slice(256 * j, 256 * (j + 1))
        for i in range(4):
            r = slice(256 * i, 256 * (i + 1))
            v = src[r, c].astype(F32)
            w = ((5.0 * eye - v) if i == j else -v) * 0.25
            dst[r, c] = w.astype(BF16)


def chain_kernel(idx, it, g, root, mixed, f0, f1, t0, t1):
    z, co = idx[0], idx[1]

    def mul(dst, a, b):
        for j in range(4):
            c = slice(256 * j, 256 * (j + 1))
            dst[:, c] = dot(a[...], b[:, c]).astype(BF16)

    negate_quarter(f0, it)
    mul(t0, f0, f0)
    mul(t1, t0, t0)
    mul(t0, t1, it)
    negate_quarter(f1, t0)
    mul(root, f0, f1)

    @pl.when(co == 0)
    def _():
        zr = pl.multiple_of(z * 128, 128)
        mixed[...] = dot(root[pl.ds(zr, 128), :], g[...]).astype(BF16)

    @pl.when(co == 1)
    def _():
        mixed[...] = jnp.zeros(mixed.shape, BF16)


def raw_kernel(mixed, root, raw, sq):
    r = dot(mixed[...], root[...])
    raw[...] = r
    sq[...] = jnp.broadcast_to(jnp.sum(r * r), sq.shape)


def sds(shape, dt):
    return jax.ShapeDtypeStruct(shape, dt)


def gather_z(x):
    up, down = [x], []
    for _ in range(4):
        up.append(shift(up[-1], "tok", Z, 1))
    for _ in range(3):
        down.append(shift((down or [x])[-1], "tok", Z, -1))
    return up + down[::-1]


def direct_z(x):
    return [x] + [shift(x, "tok", Z, d) for d in range(1, Z)]


def per_device(inputs, output_grads, statistics):
    z = lax.axis_index("tok")
    y = lax.axis_index("y")
    xl = lax.axis_index("xl")
    co = lax.axis_index("co")
    pair = lax.axis_index("pair")
    idx1 = jnp.stack([pair, xl, co, y]).astype(jnp.int32)
    idx2 = jnp.stack([z, co]).astype(jnp.int32)

    x_ring = ("xl", "pair")
    plane = ("y", "xl", "pair")
    table = []
    for yy in range(4):
        for xx in range(4):
            table.append((yy * 4 + xx, xx * 4 + yy))
    cot = lax.ppermute(output_grads, plane, table)
    a_own = [inputs] + [flip(inputs, x_ring, 4, d) for d in (1, 2, 3)]
    b = [cot] + [flip(cot, "y", 4, d) for d in (1, 2, 3)]
    a_oth = [flip(a, "co", 2, 1) for a in a_own]

    stat = statistics.reshape(128, 1024)
    wide = jnp.concatenate([stat, stat[:, :512]], axis=1)
    part = lax.dynamic_slice(wide, (0, z * 128), (128, 640))
    part = lax.ppermute(part, ("co", "pair"), [(0, 0), (1, 2), (2, 1), (3, 3)])
    st = gather_z(part)

    partial, peak = pl.pallas_call(
        partial_kernel,
        out_shape=(sds((1024, 512), F32), sds((8, 128), F32)),
        in_specs=[SMEM] + [VMEM] * 12,
        out_specs=(VMEM, VMEM),
        scratch_shapes=[pltpu.VMEM((2, 4, 512, 256), BF16), pltpu.VMEM((2, 2, 512, 256), BF16)],
        compiler_params=params(),
        name="partial_gradient",
    )(idx1, *a_own, *a_oth, *b)

    power = jnp.floor(jnp.log2(jnp.maximum(peak[:1], 1e-30)))
    up = jnp.exp2(14.0 - power)
    label = jnp.broadcast_to(power[:, :1], (16, 512)).astype(F16)
    total = lax.dynamic_slice(partial, (z * 128, 0), (128, 512))
    for d in range(1, Z):
        chunk = lax.dynamic_slice(partial, (((z + d) % Z) * 128, 0), (128, 512))
        sent = jnp.concatenate([(chunk * up[:, :1]).astype(F16), label], axis=0)
        got = shift(sent, "tok", Z, d)
        down = jnp.exp2(got[128:129, :1].astype(F32) - 14.0)
        total = total + got[:128].astype(F32) * down
    g_mine = total.astype(BF16)

    g_own = gather_z(g_mine)
    g_oth = [flip(g, "co", 2, 1) for g in g_own]

    grad, iterate, rows, grad_sq = pl.pallas_call(
        stats_kernel,
        out_shape=(sds((1024, 1024), BF16), sds((1024, 1024), BF16), sds((128, 1024), F32), sds((8, 128), F32)),
        in_specs=[SMEM] + [VMEM] * 24,
        out_specs=(VMEM,) * 4,
        scratch_shapes=[pltpu.VMEM((8, 1024, 128), F32)],
        compiler_params=params(),
        name="new_statistics",
    )(idx2, *g_own, *g_oth, *st)

    new_rows = lax.ppermute(rows, ("co", "pair"), [(0, 0), (1, 2), (2, 1), (3, 3)])

    root, mixed = pl.pallas_call(
        chain_kernel,
        out_shape=(sds((1024, 1024), BF16), sds((128, 1024), BF16)),
        in_specs=[SMEM, VMEM, VMEM],
        out_specs=(VMEM, VMEM),
        scratch_shapes=[pltpu.VMEM((1024, 1024), BF16)] * 4,
        compiler_params=params(),
        name="inverse_root",
    )(idx2, iterate, grad)

    left = lax.ppermute(mixed, "co", [(0, 1)])
    raw, raw_sq = pl.pallas_call(
        raw_kernel,
        out_shape=(sds((128, 1024), F32), sds((8, 128), F32)),
        in_specs=[VMEM, VMEM],
        out_specs=(VMEM, VMEM),
        compiler_params=params(),
        name="raw_update",
    )(left, root)

    update_sq = raw_sq
    for d in range(1, Z):
        update_sq = update_sq + shift(raw_sq, "tok", Z, d)
    ratio = jnp.sqrt(grad_sq / (update_sq + 1e-6))[:1, :1]
    final = (raw * ratio).astype(BF16)
    lo = lax.ppermute(final[:64], ("co", "pair"), [(2, 0), (3, 2)])
    hi = lax.ppermute(final[64:], ("co", "pair"), [(2, 1), (3, 3)])
    update = jnp.where(pair == 0, lo, hi)
    return update[None], new_rows[None, None]


def solution(mesh):
    m = Mesh(mesh.devices.reshape(8, 4, 2, 2, 2), ("tok", "y", "xl", "co", "pair"))
    tile = ("y", "xl", "co")
    return jax.shard_map(
        per_device,
        mesh=m,
        in_specs=(P(("tok", "pair"), tile), P(("tok", "pair"), tile), P(tile, "pair", "tok", None)),
        out_specs=(P(tile, ("tok", "pair"), None), P(tile, "pair", "tok", None)),
        check_vma=False,
    )
```

```python
import jax
import jax.numpy as jnp
from jax import lax
from jax.experimental import pallas as pl
from jax.experimental.pallas import tpu as pltpu
from jax.sharding import Mesh, PartitionSpec as P


F32 = jnp.float32
BF16 = jnp.bfloat16
F16 = jnp.float16
VMEM = pl.BlockSpec(memory_space=pltpu.VMEM)
SMEM = pl.BlockSpec(memory_space=pltpu.SMEM)
Z = 8
SWAP = [(0, 0), (1, 2), (2, 1), (3, 3)]


def params(mib):
    return pltpu.CompilerParams(vmem_limit_bytes=mib * 1024 * 1024)


def sds(shape, dt):
    return jax.ShapeDtypeStruct(shape, dt)


def dot(a, b, ca=1, cb=0):
    return lax.dot_general(a, b, (((ca,), (cb,)), ((), ())), preferred_element_type=F32)


def cat(ref):
    return jnp.concatenate([ref[k] for k in range(ref.shape[0])], axis=1)


def loop(n, body):
    lax.fori_loop(0, n, lambda j, c: (body(j), c)[1], 0)


def diagonal(n):
    return lax.broadcasted_iota(jnp.int32, (n, n), 0) == lax.broadcasted_iota(jnp.int32, (n, n), 1)


def partial_kernel(idx, a_own, a_oth, b, out, peak, top):
    co = idx[0]
    top[...] = jnp.zeros(top.shape, F32)
    for ref, c in ((a_own, co), (a_oth, 1 - co)):
        for l in range(2):
            r = pl.multiple_of(256 * (2 * l + c), 256)
            for cb in range(2):
                acc = dot(ref[2 * l], b[2 * cb], 0, 0) + dot(ref[2 * l + 1], b[2 * cb + 1], 0, 0)
                out[pl.ds(r, 256), 256 * cb:256 * (cb + 1)] = acc
                top[...] = jnp.maximum(top[...], jnp.max(jnp.abs(acc), axis=0, keepdims=True))
    peak[...] = jnp.broadcast_to(jnp.max(top[...]), peak.shape)


def chain_kernel(idx, st, g0, r1, r2, r3, r4, o1, o2, o3, o4,
                 root, grad, rows, s_s, x_s, before, f0, f1, t0, t1):
    z, co = idx[0], idx[1]
    step = 1 - 2 * co
    pieces = [(g0, z, 0), (r1, z - step, 0), (r2, z - 2 * step, 0), (r3, z - 3 * step, 0),
              (o1, z + step, 0), (o2, z + 2 * step, 0), (o3, z + 3 * step, 0),
              (r4, z + 4, 64 * co), (o4, z + 4, 64 * (1 - co))]
    for ref, src, off in pieces:
        n = ref.shape[1]
        blk = (src + 2 * Z) % Z
        r = pl.multiple_of(blk * 128 + off, 64)
        for c in range(2):
            for cb in range(2):
                grad[2 * cb + c, pl.ds(r, n), :] = ref[c, :, 256 * cb:256 * (cb + 1)]

    @pl.when(co == 0)
    def _():
        for j in range(4):
            x_s[2 * j] = grad[j, :, :128]
            x_s[2 * j + 1] = grad[j, :, 128:]

    @pl.when(co == 1)
    def _():
        def body(k):
            r = pl.multiple_of(k * 128, 128)
            for j in range(4):
                x_s[k, 256 * j:256 * (j + 1), :] = grad[j, pl.ds(r, 128), :].T
        loop(Z, body)

    def spread(rb):
        r = pl.multiple_of(rb * 128, 128)
        for k in range(5):
            cb = (rb + k) % Z
            c = pl.multiple_of(cb * 128, 128)
            blk = st[rb, :, 128 * k:128 * (k + 1)]
            s_s[cb, pl.ds(r, 128), :] = blk
            if 0 < k < 4:
                s_s[rb, pl.ds(c, 128), :] = blk.T
    loop(Z, spread)

    zr = pl.multiple_of(z * 128, 128)
    for j in range(Z):
        before[:, 128 * j:128 * (j + 1)] = s_s[j, pl.ds(zr, 128), :]

    def product(j):
        r = pl.multiple_of(j * 256, 256)
        p = dot(cat(x_s), jnp.concatenate([x_s[k, pl.ds(r, 256), :] for k in range(Z)], axis=1), 1, 1)
        s_s[2 * j] = s_s[2 * j] + 0.1 * p[:, :128]
        s_s[2 * j + 1] = s_s[2 * j + 1] + 0.1 * p[:, 128:]
    loop(4, product)

    for j in range(Z):
        c = slice(128 * j, 128 * (j + 1))
        rows[:, c] = s_s[j, pl.ds(zr, 128), :] - before[:, c]
    top = None
    for j in range(Z):
        m = jnp.sum(jnp.abs(s_s[j]), axis=0, keepdims=True)
        top = m if top is None else jnp.maximum(top, m)
    bound = jnp.max(top, axis=1, keepdims=True)
    inv = 1.0 / (1.1 * bound)
    ridge = jnp.where(diagonal(128), 0.1 * bound, 0.0)
    five = jnp.where(diagonal(256), 5.0, 0.0)

    def first(j):
        for h in range(2):
            lo = pl.multiple_of(256 * j + 128 * h, 128)
            c = slice(128 * h, 128 * (h + 1))
            t1[j, :, c] = (s_s[2 * j + h] * inv).astype(BF16)
            t1[j, pl.ds(lo, 128), c] = ((s_s[2 * j + h, pl.ds(lo, 128), :] + ridge) * inv).astype(BF16)
        r = pl.multiple_of(256 * j, 256)
        f0[j] = t1[j] * jnp.asarray(-0.25, BF16)
        f0[j, pl.ds(r, 256), :] = ((five - t1[j, pl.ds(r, 256), :].astype(F32)) * 0.25).astype(BF16)
    loop(4, first)

    def mul(dst, a, b):
        def body(j):
            dst[j] = dot(cat(a), b[j]).astype(BF16)
        loop(4, body)

    mul(t0, f0, f0)
    mul(f1, t0, t0)

    def second(j):
        r = pl.multiple_of(256 * j, 256)
        t0[j] = dot(cat(f1), t1[j]).astype(BF16)
        diag = ((five - t0[j, pl.ds(r, 256), :].astype(F32)) * 0.25).astype(BF16)
        t0[j] = t0[j] * jnp.asarray(-0.25, BF16)
        t0[j, pl.ds(r, 256), :] = diag
    loop(4, second)
    mul(root, f0, t0)


def update_kernel(idx, own, other, grad, out, mix, r_s, keep):
    z, co = idx[0], idx[1]
    zr = pl.multiple_of(z * 128 + co * 64, 64)

    def run(left, right):
        def mixed(j):
            mix[j] = dot(cat(left), grad[j]).astype(BF16)
        loop(4, mixed)

        def raw(j, acc):
            r = dot(cat(mix), right[j])
            r_s[...] = r
            keep[j] = r_s[pl.ds(zr, 64), :]
            return acc + jnp.sum(r * r, axis=0, keepdims=True)
        update_sq = jnp.sum(lax.fori_loop(0, 4, raw, jnp.zeros((1, 256), F32)), axis=1, keepdims=True)

        def square(j, acc):
            v = grad[j].astype(F32)
            return acc + jnp.sum(v * v, axis=0, keepdims=True)
        grad_sq = jnp.sum(lax.fori_loop(0, 4, square, jnp.zeros((1, 256), F32)), axis=1, keepdims=True)
        ratio = jnp.sqrt(grad_sq / (update_sq + 1e-6))
        for j in range(4):
            out[:, 256 * j:256 * (j + 1)] = (keep[j] * ratio).astype(BF16)

    pl.when(co == 0)(lambda: run(own, other))
    pl.when(co == 1)(lambda: run(other, own))


def pack(x, peak):
    power = jnp.floor(jnp.log2(jnp.maximum(peak, 1e-30)))
    scaled = (x * jnp.exp2(14.0 - power)).astype(F16)
    label = jnp.broadcast_to(power, (*x.shape[:-2], 16, x.shape[-1])).astype(F16)
    return jnp.concatenate([scaled, label], axis=-2)


def unpack(x):
    return x[:, :-16].astype(F32) * jnp.exp2(x[:, -16:-15, :1].astype(F32) - 14.0)


def everyone(x, axis, n):
    return lax.all_to_all(jnp.broadcast_to(x, (n, *x.shape)), axis, 0, 0, tiled=True)


def sibling(x):
    return lax.ppermute(x, "co", [(0, 1), (1, 0)])


def per_device(inputs, output_grads, statistics):
    z = lax.axis_index("tok")
    co = lax.axis_index("co")
    idx1 = jnp.stack([co, z]).astype(jnp.int32)
    idx2 = jnp.stack([z, co]).astype(jnp.int32)

    table = [(yy * 4 + xx, xx * 4 + yy) for yy in range(4) for xx in range(4)]
    cot = lax.ppermute(output_grads, ("y", "xl", "pair"), table)
    a_own = everyone(inputs.reshape(512, 256), ("xl", "pair"), 4)
    b = everyone(cot, "y", 4)
    a_oth = sibling(a_own)

    stat = statistics.reshape(128, 1024)
    wide = jnp.concatenate([stat, stat[:, :512]], axis=1)
    part = lax.dynamic_slice(wide, (0, z * 128), (128, 640))
    part = pack(part, jnp.max(jnp.abs(stat)))
    part = lax.ppermute(part, ("co", "pair"), SWAP)
    st = 0.9 * unpack(everyone(part, "tok", Z))

    partial, peak = pl.pallas_call(
        partial_kernel,
        out_shape=(sds((1024, 512), F32), sds((8, 128), F32)),
        in_specs=[SMEM] + [VMEM] * 3,
        out_specs=(VMEM, VMEM),
        scratch_shapes=[pltpu.VMEM((1, 256), F32)],
        compiler_params=params(14),
        name="partial_gradient",
    )(idx1, a_own, a_oth, b)

    sent = pack(partial.reshape(Z, 128, 512), peak[0, 0])
    got = lax.all_to_all(sent, "tok", 0, 0, tiled=True)
    mine = jnp.sum(unpack(got), axis=0).astype(BF16)
    theirs = sibling(mine)
    piece = jnp.where(co == 0, jnp.stack([mine, theirs]), jnp.stack([theirs, mine]))
    ring = []
    for i in range(Z):
        ring += [(2 * i, 2 * ((i + 1) % Z)), (2 * i + 1, 2 * ((i - 1) % Z) + 1)]
    runs, others = [piece], []
    for s in range(1, 5):
        src = runs[-1]
        if s == 4:
            src = lax.dynamic_slice_in_dim(src, co * 64, 64, 1)
        runs.append(lax.ppermute(src, ("tok", "co"), ring))
        others.append(sibling(runs[-1]))

    root, grad, rows = pl.pallas_call(
        chain_kernel,
        out_shape=(sds((4, 1024, 256), BF16), sds((4, 1024, 256), BF16), sds((128, 1024), F32)),
        in_specs=[SMEM] + [VMEM] * 10,
        out_specs=(VMEM,) * 3,
        scratch_shapes=[pltpu.VMEM((8, 1024, 128), F32), pltpu.VMEM((8, 1024, 128), BF16),
                        pltpu.VMEM((128, 1024), F32)] + [pltpu.VMEM((4, 1024, 256), BF16)] * 4,
        compiler_params=params(34),
        name="inverse_root",
    )(idx2, st, *runs, *others)

    other_root = sibling(root)
    back = lax.ppermute(rows, ("co", "pair"), SWAP)
    final = pl.pallas_call(
        update_kernel,
        out_shape=sds((64, 1024), BF16),
        in_specs=[SMEM] + [VMEM] * 3,
        out_specs=VMEM,
        scratch_shapes=[pltpu.VMEM((4, 1024, 256), BF16), pltpu.VMEM((1024, 256), F32), pltpu.VMEM((4, 64, 256), F32)],
        compiler_params=params(16),
        name="update_rows",
    )(idx2, root, other_root, grad)
    update = lax.ppermute(final, ("co", "pair"), SWAP)
    new_rows = 0.9 * stat + back
    return update[None], new_rows[None, None]


def solution(mesh):
    m = Mesh(mesh.devices.reshape(8, 4, 2, 2, 2), ("tok", "y", "xl", "co", "pair"))
    tile = ("y", "xl", "co")
    return jax.shard_map(
        per_device,
        mesh=m,
        in_specs=(P(("tok", "pair"), tile), P(("tok", "pair"), tile), P(tile, "pair", "tok", None)),
        out_specs=(P(tile, ("tok", "pair"), None), P(tile, "pair", "tok", None)),
        check_vma=False,
    )
```

```python
import jax
import jax.numpy as jnp
from jax import lax
from jax.experimental import pallas as pl
from jax.experimental.pallas import tpu as pltpu
from jax.sharding import Mesh, PartitionSpec as P


F32 = jnp.float32
BF16 = jnp.bfloat16
F16 = jnp.float16
VMEM = pl.BlockSpec(memory_space=pltpu.VMEM)
SMEM = pl.BlockSpec(memory_space=pltpu.SMEM)
HBM = pl.BlockSpec(memory_space=pltpu.HBM)
Z = 8
SWAP = [(0, 0), (1, 2), (2, 1), (3, 3)]


def params(mib):
    return pltpu.CompilerParams(vmem_limit_bytes=mib * 1024 * 1024)


def sds(shape, dt):
    return jax.ShapeDtypeStruct(shape, dt)


def dot(a, b, ca=1, cb=0):
    return lax.dot_general(a, b, (((ca,), (cb,)), ((), ())), preferred_element_type=F32)


def cat(ref):
    return jnp.concatenate([ref[k] for k in range(ref.shape[0])], axis=1)


def loop(n, body):
    lax.fori_loop(0, n, lambda j, c: (body(j), c)[1], 0)


def diagonal(n):
    return lax.broadcasted_iota(jnp.int32, (n, n), 0) == lax.broadcasted_iota(jnp.int32, (n, n), 1)


def partial_kernel(idx, *refs):
    a_own, a_oth, (b, out, acc_s, top) = refs[:4], refs[4:8], refs[8:]
    co, xl, pair = idx[0], idx[2], idx[3]
    top[...] = jnp.zeros(top.shape, F32)
    for h in range(2):
        for ref, c in ((a_own, co), (a_oth, 1 - co)):
            r = pl.multiple_of(256 * (2 * (xl ^ h) + c), 256)
            for cb in range(2):
                acc = (dot(ref[2 * h][...], b[2 * cb + pair], 0, 0)
                       + dot(ref[2 * h + 1][...], b[2 * cb + 1 - pair], 0, 0))
                acc_s[pl.ds(r, 256), 256 * cb:256 * (cb + 1)] = acc
                top[...] = jnp.maximum(top[...], jnp.max(jnp.abs(acc), axis=0, keepdims=True))
    peak = jnp.max(top[...], axis=1, keepdims=True)
    power = jnp.floor(jnp.log2(jnp.maximum(peak, 1e-30)))
    up = jnp.exp2(14.0 - power)

    def body(k):
        out[k, :128, :] = acc_s[pl.ds(pl.multiple_of(128 * k, 128), 128), :] * up
        out[k, 128:, :] = jnp.broadcast_to(power, (16, 512))

    loop(Z, body)


def assemble_kernel(idx, *refs):
    pieces, s_out = refs[:Z], refs[Z]
    z = idx[0]
    for d in range(Z):
        rb = (z + Z - d) % Z
        r = pl.multiple_of(rb * 128, 128)
        for k in range(5):
            cb = (rb + k) % Z
            c = pl.multiple_of(cb * 128, 128)
            blk = pieces[d][:, 128 * k:128 * (k + 1)]
            s_out[cb, pl.ds(r, 128), :] = blk
            if 0 < k < 4:
                s_out[rb, pl.ds(c, 128), :] = blk.T


def chain_kernel(idx, st, g0, r1, r2, r3, r4, o1, o2, o3, o4,
                 root, grad, rows, s_s, x_s, before, f0, f1, t0, t1, sem):
    z, co = idx[0], idx[1]
    fetch = pltpu.make_async_copy(st, s_s, sem)
    fetch.start()
    step = 1 - 2 * co
    pieces = [(g0, z, 0), (r1, z - step, 0), (r2, z - 2 * step, 0), (r3, z - 3 * step, 0),
              (o1, z + step, 0), (o2, z + 2 * step, 0), (o3, z + 3 * step, 0),
              (r4, z + 4, 64 * co), (o4, z + 4, 64 * (1 - co))]
    for ref, src, off in pieces:
        n = ref.shape[1]
        blk = (src + 2 * Z) % Z
        r = pl.multiple_of(blk * 128 + off, 64)
        for c in range(2):
            for cb in range(2):
                grad[2 * cb + c, pl.ds(r, n), :] = ref[c, :, 256 * cb:256 * (cb + 1)]

    @pl.when(co == 0)
    def _():
        for j in range(4):
            x_s[2 * j] = grad[j, :, :128]
            x_s[2 * j + 1] = grad[j, :, 128:]

    @pl.when(co == 1)
    def _():
        def body(k):
            r = pl.multiple_of(k * 128, 128)
            for j in range(4):
                x_s[k, 256 * j:256 * (j + 1), :] = grad[j, pl.ds(r, 128), :].T

        loop(Z, body)

    fetch.wait()
    zr = pl.multiple_of(z * 128, 128)
    for j in range(Z):
        before[:, 128 * j:128 * (j + 1)] = s_s[j, pl.ds(zr, 128), :]

    def product(j):
        r = pl.multiple_of(j * 256, 256)
        p = dot(cat(x_s), jnp.concatenate([x_s[k, pl.ds(r, 256), :] for k in range(Z)], axis=1), 1, 1)
        s_s[2 * j] = s_s[2 * j] + 0.1 * p[:, :128]
        s_s[2 * j + 1] = s_s[2 * j + 1] + 0.1 * p[:, 128:]

    loop(4, product)

    for j in range(Z):
        c = slice(128 * j, 128 * (j + 1))
        rows[:, c] = s_s[j, pl.ds(zr, 128), :] - before[:, c]
    top = None
    for j in range(Z):
        m = jnp.sum(jnp.abs(s_s[j]), axis=0, keepdims=True)
        top = m if top is None else jnp.maximum(top, m)
    bound = jnp.max(top, axis=1, keepdims=True)
    inv = 1.0 / (1.1 * bound)
    ridge = jnp.where(diagonal(128), 0.1 * bound, 0.0)
    five = jnp.where(diagonal(256), 5.0, 0.0)

    def first(j):
        for h in range(2):
            lo = pl.multiple_of(256 * j + 128 * h, 128)
            c = slice(128 * h, 128 * (h + 1))
            t1[j, :, c] = (s_s[2 * j + h] * inv).astype(BF16)
            t1[j, pl.ds(lo, 128), c] = ((s_s[2 * j + h, pl.ds(lo, 128), :] + ridge) * inv).astype(BF16)
        r = pl.multiple_of(256 * j, 256)
        f0[j] = t1[j] * jnp.asarray(-0.25, BF16)
        f0[j, pl.ds(r, 256), :] = ((five - t1[j, pl.ds(r, 256), :].astype(F32)) * 0.25).astype(BF16)

    loop(4, first)

    def mul(dst, a, b):
        def body(j):
            dst[j] = dot(cat(a), b[j]).astype(BF16)

        loop(4, body)

    mul(t0, f0, f0)
    mul(f1, t0, t0)

    def second(j):
        r = pl.multiple_of(256 * j, 256)
        t0[j] = dot(cat(f1), t1[j]).astype(BF16)
        diag = ((five - t0[j, pl.ds(r, 256), :].astype(F32)) * 0.25).astype(BF16)
        t0[j] = t0[j] * jnp.asarray(-0.25, BF16)
        t0[j, pl.ds(r, 256), :] = diag

    loop(4, second)
    mul(root, f0, t0)


def update_kernel(idx, own, other, grad, out, mix, r_s, keep):
    z, co = idx[0], idx[1]
    zr = pl.multiple_of(z * 128 + co * 64, 64)

    def run(left, right):
        def mixed(j):
            mix[j] = dot(cat(left), grad[j]).astype(BF16)

        loop(4, mixed)

        def raw(j, acc):
            r = dot(cat(mix), right[j])
            r_s[...] = r
            keep[j] = r_s[pl.ds(zr, 64), :]
            return acc + jnp.sum(r * r, axis=0, keepdims=True)

        update_sq = jnp.sum(lax.fori_loop(0, 4, raw, jnp.zeros((1, 256), F32)), axis=1, keepdims=True)

        def square(j, acc):
            v = grad[j].astype(F32)
            return acc + jnp.sum(v * v, axis=0, keepdims=True)

        grad_sq = jnp.sum(lax.fori_loop(0, 4, square, jnp.zeros((1, 256), F32)), axis=1, keepdims=True)
        ratio = jnp.sqrt(grad_sq / (update_sq + 1e-6))
        for j in range(4):
            out[:, 256 * j:256 * (j + 1)] = (keep[j] * ratio).astype(BF16)

    pl.when(co == 0)(lambda: run(own, other))
    pl.when(co == 1)(lambda: run(other, own))


def pack(x, peak):
    power = jnp.floor(jnp.log2(jnp.maximum(peak, 1e-30)))
    scaled = (x * jnp.exp2(14.0 - power)).astype(F16)
    label = jnp.broadcast_to(power, (*x.shape[:-2], 16, x.shape[-1])).astype(F16)
    return jnp.concatenate([scaled, label], axis=-2)


def unpack(x):
    return x[..., :-16, :].astype(F32) * jnp.exp2(x[..., -16:-15, :].astype(F32) - 14.0)


def everyone(x, axis, n):
    return lax.all_to_all(jnp.broadcast_to(x, (n, *x.shape)), axis, 0, 0, tiled=True)


def sibling(x):
    return lax.ppermute(x, "co", [(0, 1), (1, 0)])


def around(x):
    up, down = [x], []
    for k in range(1, 5):
        up.append(lax.ppermute(up[-1], "tok", [(i, (i + 1) % Z) for i in range(Z)]))
        if k < 4:
            down.append(lax.ppermute((down or [x])[-1], "tok", [(i, (i - 1) % Z) for i in range(Z)]))
    return up + down[::-1]


def step(inputs, output_grads, statistics):
    z = lax.axis_index("tok")
    co = lax.axis_index("co")
    idx1 = jnp.stack([co, z, lax.axis_index("xl"), lax.axis_index("pair")]).astype(jnp.int32)
    idx2 = jnp.stack([z, co]).astype(jnp.int32)

    table = [(yy * 4 + xx, xx * 4 + yy) for yy in range(4) for xx in range(4)]
    cot = lax.ppermute(output_grads, ("y", "xl", "pair"), table)
    a_own = [inputs]
    for d in range(1, 4):
        a_own.append(lax.ppermute(inputs, ("xl", "pair"), [(i, i ^ d) for i in range(4)]))
    b = everyone(cot, "y", 4)
    a_oth = []
    for d in range(4):
        a_oth.append(sibling(a_own[d]))

    stat = statistics.reshape(128, 1024)
    wide = jnp.concatenate([stat, stat[:, :512]], axis=1)
    part = lax.dynamic_slice(wide, (0, z * 128), (128, 640))
    part = pack(part, jnp.max(jnp.abs(stat)))
    part = lax.ppermute(part, ("co", "pair"), SWAP)
    st = around(part)
    st = pl.pallas_call(
        assemble_kernel,
        out_shape=sds((8, 1024, 128), F32),
        in_specs=[SMEM] + [VMEM] * Z,
        out_specs=VMEM,
        compiler_params=params(10),
        name="assemble",
    )(idx2, *[0.9 * unpack(p) for p in st])

    partial = pl.pallas_call(
        partial_kernel,
        out_shape=sds((Z, 144, 512), F32),
        in_specs=[SMEM] + [VMEM] * 9,
        out_specs=VMEM,
        scratch_shapes=[pltpu.VMEM((1024, 512), F32), pltpu.VMEM((1, 256), F32)],
        compiler_params=params(14),
        name="partial_gradient",
    )(idx1, *a_own, *a_oth, b)

    got = lax.all_to_all(partial.astype(F16), "tok", 0, 0, tiled=True)
    mine = jnp.sum(unpack(got), axis=0).astype(BF16)
    theirs = sibling(mine)
    piece = jnp.where(co == 0, jnp.stack([mine, theirs]), jnp.stack([theirs, mine]))
    ring = []
    for i in range(Z):
        ring += [(2 * i, 2 * ((i + 1) % Z)), (2 * i + 1, 2 * ((i - 1) % Z) + 1)]
    runs, others = [piece], []
    for s in range(1, 5):
        src = runs[-1]
        if s == 4:
            src = lax.dynamic_slice_in_dim(src, co * 64, 64, 1)
        runs.append(lax.ppermute(src, ("tok", "co"), ring))
        others.append(sibling(runs[-1]))

    root, grad, rows = pl.pallas_call(
        chain_kernel,
        out_shape=(sds((4, 1024, 256), BF16), sds((4, 1024, 256), BF16), sds((128, 1024), F32)),
        in_specs=[SMEM, HBM] + [VMEM] * 9,
        out_specs=(VMEM,) * 3,
        scratch_shapes=[pltpu.VMEM((8, 1024, 128), F32), pltpu.VMEM((8, 1024, 128), BF16),
                        pltpu.VMEM((128, 1024), F32)] + [pltpu.VMEM((4, 1024, 256), BF16)] * 4
        + [pltpu.SemaphoreType.DMA],
        compiler_params=params(22),
        name="inverse_root",
    )(idx2, st, *runs, *others)

    other_root = sibling(root)
    back = lax.ppermute(rows, ("co", "pair"), SWAP)
    final = pl.pallas_call(
        update_kernel,
        out_shape=sds((64, 1024), BF16),
        in_specs=[SMEM] + [VMEM] * 3,
        out_specs=VMEM,
        scratch_shapes=[pltpu.VMEM((4, 1024, 256), BF16), pltpu.VMEM((1024, 256), F32), pltpu.VMEM((4, 64, 256), F32)],
        compiler_params=params(16),
        name="update_rows",
    )(idx2, root, other_root, grad)
    update = lax.ppermute(final, ("co", "pair"), SWAP)
    new_rows = 0.9 * stat + back
    return update[None], new_rows[None, None]


def solution(mesh):
    m = Mesh(mesh.devices.reshape(8, 4, 2, 2, 2), ("tok", "y", "xl", "co", "pair"))
    tile = ("y", "xl", "co")
    return jax.shard_map(
        step,
        mesh=m,
        in_specs=(P(("tok", "pair"), tile), P(("tok", "pair"), tile), P(tile, "pair", "tok", None)),
        out_specs=(P(tile, ("tok", "pair"), None), P(tile, "pair", "tok", None)),
        check_vma=False,
    )
```

```python
import jax
import jax.numpy as jnp
from jax import lax
from jax.experimental import pallas as pl
from jax.experimental.pallas import tpu as pltpu
from jax.sharding import Mesh, PartitionSpec as P


F32 = jnp.float32
BF16 = jnp.bfloat16
F16 = jnp.float16
VMEM = pl.BlockSpec(memory_space=pltpu.VMEM)
SMEM = pl.BlockSpec(memory_space=pltpu.SMEM)
HBM = pl.BlockSpec(memory_space=pltpu.HBM)
Z = 8
SWAP = [(0, 0), (1, 2), (2, 1), (3, 3)]


def params(mib):
    return pltpu.CompilerParams(vmem_limit_bytes=mib * 1024 * 1024)


def sds(shape, dt):
    return jax.ShapeDtypeStruct(shape, dt)


def dot(a, b, ca=1, cb=0):
    return lax.dot_general(a, b, (((ca,), (cb,)), ((), ())), preferred_element_type=F32)


def cat(ref):
    return jnp.concatenate([ref[k] for k in range(ref.shape[0])], axis=1)


def loop(n, body):
    lax.fori_loop(0, n, lambda j, c: (body(j), c)[1], 0)


def diagonal(n):
    return lax.broadcasted_iota(jnp.int32, (n, n), 0) == lax.broadcasted_iota(jnp.int32, (n, n), 1)


def partial_kernel(idx, a_own, a_oth, b0, b1, b2, b3, out, acc_s, top):
    co, y = idx[0], idx[2]
    b = (b0, b1, b2, b3)
    top[...] = jnp.zeros(top.shape, F32)
    for h in range(2):
        cb = (y >> 1) ^ h
        for ref, c in ((a_own, co), (a_oth, 1 - co)):
            for l in range(2):
                r = pl.multiple_of(256 * (2 * l + c), 256)
                acc = (dot(ref[2 * l + (y & 1)], b[2 * h][...], 0, 0)
                       + dot(ref[2 * l + 1 - (y & 1)], b[2 * h + 1][...], 0, 0))
                acc_s[cb, pl.ds(r, 256), :] = acc
                top[...] = jnp.maximum(top[...], jnp.max(jnp.abs(acc), axis=0, keepdims=True))
    peak = jnp.max(top[...], axis=1, keepdims=True)
    power = jnp.floor(jnp.log2(jnp.maximum(peak, 1e-30)))
    up = jnp.exp2(14.0 - power)

    def body(k):
        r = pl.multiple_of(128 * k, 128)
        for cb in range(2):
            out[k, :128, 256 * cb:256 * (cb + 1)] = acc_s[cb, pl.ds(r, 128), :] * up
        out[k, 128:, :] = jnp.broadcast_to(power, (16, 512))

    loop(Z, body)


def assemble_kernel(idx, pieces, s_out):
    z = idx[0]
    for d in range(Z):
        rb = (z + Z - d) % Z
        r = pl.multiple_of(rb * 128, 128)
        for k in range(5):
            cb = (rb + k) % Z
            c = pl.multiple_of(cb * 128, 128)
            blk = pieces[d, :, 128 * k:128 * (k + 1)]
            s_out[cb, pl.ds(r, 128), :] = blk
            if 0 < k < 4:
                s_out[rb, pl.ds(c, 128), :] = blk.T


def merge_kernel(idx, mine, theirs, out):
    co = idx[1]
    out[co] = mine[...]
    out[1 - co] = theirs[...]


def half_kernel(idx, src, out):
    out[...] = src[:, pl.ds(pl.multiple_of(64 * idx[1], 64), 64), :]


def chain_kernel(idx, st, g0, r1, r2, r3, r4, o1, o2, o3, o4,
                 root, grad, rows, s_s, x_s, before, f0, f1, t0, t1, sem):
    z, co = idx[0], idx[1]
    fetch = pltpu.make_async_copy(st, s_s, sem)
    fetch.start()
    step = 1 - 2 * co
    pieces = [(g0, z, 0), (r1, z - step, 0), (r2, z - 2 * step, 0), (r3, z - 3 * step, 0),
              (o1, z + step, 0), (o2, z + 2 * step, 0), (o3, z + 3 * step, 0),
              (r4, z + 4, 64 * co), (o4, z + 4, 64 * (1 - co))]
    for ref, src, off in pieces:
        n = ref.shape[1]
        blk = (src + 2 * Z) % Z
        r = pl.multiple_of(blk * 128 + off, 64)
        for c in range(2):
            for cb in range(2):
                grad[2 * cb + c, pl.ds(r, n), :] = ref[c, :, 256 * cb:256 * (cb + 1)]

    @pl.when(co == 0)
    def _():
        for j in range(4):
            x_s[2 * j] = grad[j, :, :128]
            x_s[2 * j + 1] = grad[j, :, 128:]

    @pl.when(co == 1)
    def _():
        def body(k):
            r = pl.multiple_of(k * 128, 128)
            for j in range(4):
                x_s[k, 256 * j:256 * (j + 1), :] = grad[j, pl.ds(r, 128), :].T

        loop(Z, body)

    fetch.wait()
    zr = pl.multiple_of(z * 128, 128)
    for j in range(Z):
        before[:, 128 * j:128 * (j + 1)] = s_s[j, pl.ds(zr, 128), :]

    def product(j):
        r = pl.multiple_of(j * 256, 256)
        p = dot(cat(x_s), jnp.concatenate([x_s[k, pl.ds(r, 256), :] for k in range(Z)], axis=1), 1, 1)
        s_s[2 * j] = s_s[2 * j] + 0.1 * p[:, :128]
        s_s[2 * j + 1] = s_s[2 * j + 1] + 0.1 * p[:, 128:]

    loop(4, product)

    for j in range(Z):
        c = slice(128 * j, 128 * (j + 1))
        rows[:, c] = s_s[j, pl.ds(zr, 128), :] - before[:, c]
    top = None
    for j in range(Z):
        m = jnp.sum(jnp.abs(s_s[j]), axis=0, keepdims=True)
        top = m if top is None else jnp.maximum(top, m)
    bound = jnp.max(top, axis=1, keepdims=True)
    inv = 1.0 / (1.1 * bound)
    ridge = jnp.where(diagonal(128), 0.1 * bound, 0.0)
    five = jnp.where(diagonal(256), 5.0, 0.0)

    def first(j):
        for h in range(2):
            lo = pl.multiple_of(256 * j + 128 * h, 128)
            c = slice(128 * h, 128 * (h + 1))
            t1[j, :, c] = (s_s[2 * j + h] * inv).astype(BF16)
            t1[j, pl.ds(lo, 128), c] = ((s_s[2 * j + h, pl.ds(lo, 128), :] + ridge) * inv).astype(BF16)
        r = pl.multiple_of(256 * j, 256)
        f0[j] = t1[j] * jnp.asarray(-0.25, BF16)
        f0[j, pl.ds(r, 256), :] = ((five - t1[j, pl.ds(r, 256), :].astype(F32)) * 0.25).astype(BF16)

    loop(4, first)

    def mul(dst, a, b):
        def body(j):
            dst[j] = dot(cat(a), b[j]).astype(BF16)

        loop(4, body)

    mul(t0, f0, f0)
    mul(f1, t0, t0)

    def second(j):
        r = pl.multiple_of(256 * j, 256)
        t0[j] = dot(cat(f1), t1[j]).astype(BF16)
        diag = ((five - t0[j, pl.ds(r, 256), :].astype(F32)) * 0.25).astype(BF16)
        t0[j] = t0[j] * jnp.asarray(-0.25, BF16)
        t0[j, pl.ds(r, 256), :] = diag

    loop(4, second)
    mul(root, f0, t0)


def update_kernel(idx, own, other, grad, out, mix, r_s, keep):
    z, co = idx[0], idx[1]
    zr = pl.multiple_of(z * 128 + co * 64, 64)

    def run(left, right):
        def mixed(j):
            mix[j] = dot(cat(left), grad[j]).astype(BF16)

        loop(4, mixed)

        def raw(j, acc):
            r = dot(cat(mix), right[j])
            r_s[...] = r
            keep[j] = r_s[pl.ds(zr, 64), :]
            return acc + jnp.sum(r * r, axis=0, keepdims=True)

        update_sq = jnp.sum(lax.fori_loop(0, 4, raw, jnp.zeros((1, 256), F32)), axis=1, keepdims=True)

        def square(j, acc):
            v = grad[j].astype(F32)
            return acc + jnp.sum(v * v, axis=0, keepdims=True)

        grad_sq = jnp.sum(lax.fori_loop(0, 4, square, jnp.zeros((1, 256), F32)), axis=1, keepdims=True)
        ratio = jnp.sqrt(grad_sq / (update_sq + 1e-6))
        for j in range(4):
            out[:, 256 * j:256 * (j + 1)] = (keep[j] * ratio).astype(BF16)

    pl.when(co == 0)(lambda: run(own, other))
    pl.when(co == 1)(lambda: run(other, own))


def pack(x, peak):
    power = jnp.floor(jnp.log2(jnp.maximum(peak, 1e-30)))
    scaled = (x * jnp.exp2(14.0 - power)).astype(F16)
    label = jnp.broadcast_to(power, (*x.shape[:-2], 16, x.shape[-1])).astype(F16)
    return jnp.concatenate([scaled, label], axis=-2)


def unpack(x):
    return x[..., :-16, :].astype(F32) * jnp.exp2(x[..., -16:-15, :].astype(F32) - 14.0)


def everyone(x, axis, n):
    return lax.all_to_all(jnp.broadcast_to(x, (n, *x.shape)), axis, 0, 0, tiled=True)


def sibling(x):
    return lax.ppermute(x, "co", [(0, 1), (1, 0)])


def around(x):
    up, down = [x], []
    for k in range(1, 5):
        up.append(lax.ppermute(up[-1], "tok", [(i, (i + 1) % Z) for i in range(Z)]))
        if k < 4:
            down.append(lax.ppermute((down or [x])[-1], "tok", [(i, (i - 1) % Z) for i in range(Z)]))
    return up + down[::-1]


def step(inputs, output_grads, statistics):
    z = lax.axis_index("tok")
    co = lax.axis_index("co")
    idx1 = jnp.stack([co, z, lax.axis_index("y")]).astype(jnp.int32)
    idx2 = jnp.stack([z, co]).astype(jnp.int32)

    table = [(yy * 4 + xx, xx * 4 + yy) for yy in range(4) for xx in range(4)]
    cot = [lax.ppermute(output_grads, ("y", "xl", "pair"), table)]
    a_own = everyone(inputs, ("xl", "pair"), 4)
    for d in range(1, 4):
        cot.append(lax.ppermute(cot[0], "y", [(i, i ^ d) for i in range(4)]))
    a_oth = sibling(a_own)

    stat = statistics.reshape(128, 1024)
    wide = jnp.concatenate([stat, stat[:, :512]], axis=1)
    part = lax.dynamic_slice(wide, (0, z * 128), (128, 640))
    part = pack(part, jnp.max(jnp.abs(stat)))
    st = jnp.stack(around(part))
    st = lax.ppermute(st, ("co", "pair"), SWAP)
    st = pl.pallas_call(
        assemble_kernel,
        out_shape=sds((8, 1024, 128), F32),
        in_specs=[SMEM, VMEM],
        out_specs=VMEM,
        compiler_params=params(10),
        name="assemble",
    )(idx2, 0.9 * unpack(st))

    partial = pl.pallas_call(
        partial_kernel,
        out_shape=sds((Z, 144, 512), F32),
        in_specs=[SMEM] + [VMEM] * 6,
        out_specs=VMEM,
        scratch_shapes=[pltpu.VMEM((2, 1024, 256), F32), pltpu.VMEM((1, 256), F32)],
        compiler_params=params(14),
        name="partial_gradient",
    )(idx1, a_own, a_oth, *cot)

    got = lax.all_to_all(partial.astype(F16), "tok", 0, 0, tiled=True)
    mine = jnp.sum(unpack(got), axis=0).astype(BF16)
    theirs = sibling(mine)
    piece = pl.pallas_call(
        merge_kernel, out_shape=sds((2, 128, 512), BF16), in_specs=[SMEM, VMEM, VMEM], out_specs=VMEM,
        compiler_params=params(2), name="merge",
    )(idx2, mine, theirs)

    def pass_on(x, n):
        perm = []
        for i in range(Z):
            perm += [(2 * i, 2 * ((i + n) % Z)), (2 * i + 1, 2 * ((i - n) % Z) + 1)]
        return lax.ppermute(x, ("tok", "co"), perm)

    two = pass_on(piece, 2)
    one = pass_on(piece, 1)
    half = pl.pallas_call(
        half_kernel, out_shape=sds((2, 64, 512), BF16), in_specs=[SMEM, VMEM], out_specs=VMEM,
        compiler_params=params(2), name="half",
    )(idx2, two)
    runs = [piece, one, two, pass_on(two, 1), pass_on(half, 2)]
    others = [sibling(r) for r in runs[1:]]

    root, grad, rows = pl.pallas_call(
        chain_kernel,
        out_shape=(sds((4, 1024, 256), BF16), sds((4, 1024, 256), BF16), sds((128, 1024), F32)),
        in_specs=[SMEM, HBM] + [VMEM] * 9,
        out_specs=(VMEM,) * 3,
        scratch_shapes=[pltpu.VMEM((8, 1024, 128), F32), pltpu.VMEM((8, 1024, 128), BF16),
                        pltpu.VMEM((128, 1024), F32)] + [pltpu.VMEM((4, 1024, 256), BF16)] * 4
        + [pltpu.SemaphoreType.DMA],
        compiler_params=params(22),
        name="inverse_root",
    )(idx2, st, *runs, *others)

    other_root = sibling(root)
    back = lax.ppermute(rows, ("co", "pair"), SWAP)
    final = pl.pallas_call(
        update_kernel,
        out_shape=sds((64, 1024), BF16),
        in_specs=[SMEM] + [VMEM] * 3,
        out_specs=VMEM,
        scratch_shapes=[pltpu.VMEM((4, 1024, 256), BF16), pltpu.VMEM((1024, 256), F32), pltpu.VMEM((4, 64, 256), F32)],
        compiler_params=params(16),
        name="update_rows",
    )(idx2, root, other_root, grad)
    update = lax.ppermute(final, ("co", "pair"), SWAP)
    new_rows = 0.9 * stat + back
    return update[None], new_rows[None, None]


def solution(mesh):
    m = Mesh(mesh.devices.reshape(8, 4, 2, 2, 2), ("tok", "y", "xl", "co", "pair"))
    tile = ("y", "xl", "co")
    return jax.shard_map(
        step,
        mesh=m,
        in_specs=(P(("tok", "pair"), tile), P(("tok", "pair"), tile), P(tile, "pair", "tok", None)),
        out_specs=(P(tile, ("tok", "pair"), None), P(tile, "pair", "tok", None)),
        check_vma=False,
    )
```

```python
import jax
import jax.numpy as jnp
from jax import lax
from jax.experimental import pallas as pl
from jax.experimental.pallas import tpu as pltpu
from jax.sharding import Mesh, PartitionSpec as P


F32 = jnp.float32
BF16 = jnp.bfloat16
F16 = jnp.float16
VMEM = pl.BlockSpec(memory_space=pltpu.VMEM)
SMEM = pl.BlockSpec(memory_space=pltpu.SMEM)
Z = 8
SWAP = [(0, 0), (1, 2), (2, 1), (3, 3)]


def params(mib):
    return pltpu.CompilerParams(vmem_limit_bytes=mib * 1024 * 1024)


def sds(shape, dt):
    return jax.ShapeDtypeStruct(shape, dt)


def dot(a, b, ca=1, cb=0):
    return lax.dot_general(a, b, (((ca,), (cb,)), ((), ())), preferred_element_type=F32)


def cat(ref):
    return jnp.concatenate([ref[k] for k in range(ref.shape[0])], axis=1)


def loop(n, body):
    lax.fori_loop(0, n, lambda j, c: (body(j), c)[1], 0)


def diagonal(n):
    return lax.broadcasted_iota(jnp.int32, (n, n), 0) == lax.broadcasted_iota(jnp.int32, (n, n), 1)


def partial_kernel(idx, a_own, a_oth, b0, b1, b2, b3, out, acc_s, top):
    co, y = idx[0], idx[2]
    b = (b0, b1, b2, b3)
    top[...] = jnp.zeros(top.shape, F32)
    for h in range(2):
        cb = (y >> 1) ^ h
        for ref, c in ((a_own, co), (a_oth, 1 - co)):
            for l in range(2):
                r = pl.multiple_of(256 * (2 * l + c), 256)
                acc = (dot(ref[2 * l + (y & 1)], b[2 * h][...], 0, 0)
                       + dot(ref[2 * l + 1 - (y & 1)], b[2 * h + 1][...], 0, 0))
                acc_s[cb, pl.ds(r, 256), :] = acc
                top[...] = jnp.maximum(top[...], jnp.max(jnp.abs(acc), axis=0, keepdims=True))
    peak = jnp.max(top[...], axis=1, keepdims=True)
    power = jnp.floor(jnp.log2(jnp.maximum(peak, 1e-30)))
    up = jnp.exp2(14.0 - power)

    def body(k):
        r = pl.multiple_of(128 * k, 128)
        for cb in range(2):
            out[k, :128, 256 * cb:256 * (cb + 1)] = acc_s[cb, pl.ds(r, 128), :] * up
        out[k, 128:, :] = jnp.broadcast_to(power, (16, 512))

    loop(Z, body)


def assemble_kernel(idx, pieces, s_out):
    z = idx[0]
    for d in range(Z):
        rb = (z + Z - d) % Z
        r = pl.multiple_of(rb * 128, 128)
        for k in range(5):
            cb = (rb + k) % Z
            c = pl.multiple_of(cb * 128, 128)
            blk = pieces[d, :, 128 * k:128 * (k + 1)]
            s_out[cb, pl.ds(r, 128), :] = blk
            if 0 < k < 4:
                s_out[rb, pl.ds(c, 128), :] = blk.T


def merge_kernel(idx, mine, theirs, out):
    co = idx[1]
    out[co] = mine[...]
    out[1 - co] = theirs[...]


def half_kernel(idx, src, out):
    out[...] = src[:, pl.ds(pl.multiple_of(64 * idx[1], 64), 64), :]


def chain_kernel(idx, st, g0, r1, r2, r3, r4, o1, o2, o3, o4,
                 root, grad, rows, sq, s_s, x_s, f0, f1, t0, t1):
    z, co = idx[0], idx[1]
    step = 1 - 2 * co
    pieces = [(g0, z, 0), (r1, z - step, 0), (r2, z - 2 * step, 0), (r3, z - 3 * step, 0),
              (o1, z + step, 0), (o2, z + 2 * step, 0), (o3, z + 3 * step, 0),
              (r4, z + 4, 64 * co), (o4, z + 4, 64 * (1 - co))]
    for ref, src, off in pieces:
        n = ref.shape[1]
        blk = (src + 2 * Z) % Z
        r = pl.multiple_of(blk * 128 + off, 64)
        for c in range(2):
            for cb in range(2):
                grad[2 * cb + c, pl.ds(r, n), :] = ref[c, :, 256 * cb:256 * (cb + 1)]

    @pl.when(co == 0)
    def _():
        for j in range(4):
            x_s[2 * j] = grad[j, :, :128]
            x_s[2 * j + 1] = grad[j, :, 128:]

    @pl.when(co == 1)
    def _():
        def body(k):
            r = pl.multiple_of(k * 128, 128)
            for j in range(4):
                x_s[k, 256 * j:256 * (j + 1), :] = grad[j, pl.ds(r, 128), :].T

        loop(Z, body)

    zr = pl.multiple_of(z * 128, 128)

    def product(j, carry):
        top, acc = carry
        r = pl.multiple_of(j * 256, 256)
        p = dot(cat(x_s), jnp.concatenate([x_s[k, pl.ds(r, 256), :] for k in range(Z)], axis=1), 1, 1)
        for h in range(2):
            u = st[2 * j + h] + 0.1 * p[:, 128 * h:128 * (h + 1)]
            s_s[2 * j + h] = u
            top = jnp.maximum(top, jnp.sum(jnp.abs(u), axis=0, keepdims=True))
        v = grad[j].astype(F32)
        return top, acc + jnp.sum(v * v, axis=0, keepdims=True)

    top, acc = lax.fori_loop(0, 4, product, (jnp.zeros((1, 128), F32), jnp.zeros((1, 256), F32)))
    sq[...] = jnp.broadcast_to(jnp.sum(acc, axis=1, keepdims=True), sq.shape)

    for j in range(Z):
        c = slice(128 * j, 128 * (j + 1))
        rows[:, c] = s_s[j, pl.ds(zr, 128), :] - st[j, pl.ds(zr, 128), :]
    bound = jnp.max(top, axis=1, keepdims=True)
    inv = 1.0 / (1.1 * bound)
    ridge = jnp.where(diagonal(128), 0.1 * bound, 0.0)
    five = jnp.where(diagonal(256), 5.0, 0.0)

    def first(j):
        for h in range(2):
            lo = pl.multiple_of(256 * j + 128 * h, 128)
            c = slice(128 * h, 128 * (h + 1))
            t1[j, :, c] = (s_s[2 * j + h] * inv).astype(BF16)
            t1[j, pl.ds(lo, 128), c] = ((s_s[2 * j + h, pl.ds(lo, 128), :] + ridge) * inv).astype(BF16)
        r = pl.multiple_of(256 * j, 256)
        f0[j] = t1[j] * jnp.asarray(-0.25, BF16)
        f0[j, pl.ds(r, 256), :] = ((five - t1[j, pl.ds(r, 256), :].astype(F32)) * 0.25).astype(BF16)

    loop(4, first)

    def mul(dst, a, b):
        def body(j):
            dst[j] = dot(cat(a), b[j]).astype(BF16)

        loop(4, body)

    mul(t0, f0, f0)
    mul(f1, t0, t0)

    def second(j):
        r = pl.multiple_of(256 * j, 256)
        t0[j] = dot(cat(f1), t1[j]).astype(BF16)
        diag = ((five - t0[j, pl.ds(r, 256), :].astype(F32)) * 0.25).astype(BF16)
        t0[j] = t0[j] * jnp.asarray(-0.25, BF16)
        t0[j, pl.ds(r, 256), :] = diag

    loop(4, second)
    mul(root, f0, t0)


def update_kernel(idx, own, other, grad, grad_sq, out, mix, r_s, keep):
    z, co = idx[0], idx[1]
    zr = pl.multiple_of(z * 128 + co * 64, 64)

    def run(left, right):
        def mixed(j):
            mix[j] = dot(cat(left), grad[j]).astype(BF16)

        loop(4, mixed)

        def raw(j, acc):
            r = dot(cat(mix), right[j])
            r_s[...] = r
            keep[j] = r_s[pl.ds(zr, 64), :]
            return acc + jnp.sum(r * r, axis=0, keepdims=True)

        update_sq = jnp.sum(lax.fori_loop(0, 4, raw, jnp.zeros((1, 256), F32)), axis=1, keepdims=True)

        ratio = jnp.sqrt(grad_sq[:1, :1] / (update_sq + 1e-6))
        for j in range(4):
            out[:, 256 * j:256 * (j + 1)] = (keep[j] * ratio).astype(BF16)

    pl.when(co == 0)(lambda: run(own, other))
    pl.when(co == 1)(lambda: run(other, own))


def pack(x, peak):
    power = jnp.floor(jnp.log2(jnp.maximum(peak, 1e-30)))
    scaled = (x * jnp.exp2(14.0 - power)).astype(F16)
    label = jnp.broadcast_to(power, (*x.shape[:-2], 16, x.shape[-1])).astype(F16)
    return jnp.concatenate([scaled, label], axis=-2)


def unpack(x):
    return x[..., :-16, :].astype(F32) * jnp.exp2(x[..., -16:-15, :].astype(F32) - 14.0)


def everyone(x, axis, n):
    return lax.all_to_all(jnp.broadcast_to(x, (n, *x.shape)), axis, 0, 0, tiled=True)


def sibling(x):
    return lax.ppermute(x, "co", [(0, 1), (1, 0)])


def along(x, d):
    return lax.ppermute(x, "tok", [(i, (i + d) % Z) for i in range(Z)])


def step(inputs, output_grads, statistics):
    z = lax.axis_index("tok")
    co = lax.axis_index("co")
    idx1 = jnp.stack([co, z, lax.axis_index("y")]).astype(jnp.int32)
    idx2 = jnp.stack([z, co]).astype(jnp.int32)

    table = [(yy * 4 + xx, xx * 4 + yy) for yy in range(4) for xx in range(4)]
    cot = [lax.ppermute(output_grads, ("y", "xl", "pair"), table)]
    a_own = everyone(inputs, ("xl", "pair"), 4)
    for d in range(1, 4):
        cot.append(lax.ppermute(cot[0], "y", [(i, i ^ d) for i in range(4)]))
    a_oth = sibling(a_own)

    stat = statistics.reshape(128, 1024)
    wide = jnp.concatenate([stat, stat[:, :512]], axis=1)
    part = lax.dynamic_slice(wide, (0, z * 128), (128, 640))
    part = pack(part, jnp.max(jnp.abs(stat)))
    up2, down2 = along(part, 2), along(part, -2)
    up1, down1 = along(part, 1), along(part, -1)

    partial = pl.pallas_call(
        partial_kernel,
        out_shape=sds((Z, 144, 512), F32),
        in_specs=[SMEM] + [VMEM] * 6,
        out_specs=VMEM,
        scratch_shapes=[pltpu.VMEM((2, 1024, 256), F32), pltpu.VMEM((1, 256), F32)],
        compiler_params=params(14),
        name="partial_gradient",
    )(idx1, a_own, a_oth, *cot)

    near = lax.optimization_barrier((partial[0, 128:136, :128], part, up1, up2, down2, down1))[1:]
    far = [along(up2, 1), along(up2, 2), along(down2, -1)]
    st = jnp.stack([*near[:3], *far, *near[3:]])
    st = lax.ppermute(st, ("co", "pair"), SWAP)
    st = pl.pallas_call(
        assemble_kernel,
        out_shape=sds((8, 1024, 128), F32),
        in_specs=[SMEM, VMEM],
        out_specs=VMEM,
        compiler_params=params(10),
        name="assemble",
    )(idx2, 0.9 * unpack(st))

    got = lax.all_to_all(partial.astype(F16), "tok", 0, 0, tiled=True)
    mine = jnp.sum(unpack(got), axis=0).astype(BF16)
    theirs = sibling(mine)
    piece = pl.pallas_call(
        merge_kernel, out_shape=sds((2, 128, 512), BF16), in_specs=[SMEM, VMEM, VMEM], out_specs=VMEM,
        compiler_params=params(2), name="merge",
    )(idx2, mine, theirs)

    def pass_on(x, n):
        perm = []
        for i in range(Z):
            perm += [(2 * i, 2 * ((i + n) % Z)), (2 * i + 1, 2 * ((i - n) % Z) + 1)]
        return lax.ppermute(x, ("tok", "co"), perm)

    two = pass_on(piece, 2)
    one = pass_on(piece, 1)
    half = pl.pallas_call(
        half_kernel, out_shape=sds((2, 64, 512), BF16), in_specs=[SMEM, VMEM], out_specs=VMEM,
        compiler_params=params(2), name="half",
    )(idx2, two)
    runs = [piece, one, two, pass_on(two, 1), pass_on(half, 2)]
    others = [sibling(r) for r in runs[1:]]

    root, grad, rows, grad_sq = pl.pallas_call(
        chain_kernel,
        out_shape=(sds((4, 1024, 256), BF16), sds((4, 1024, 256), BF16), sds((128, 1024), F32), sds((8, 128), F32)),
        in_specs=[SMEM] + [VMEM] * 10,
        out_specs=(VMEM,) * 4,
        scratch_shapes=[pltpu.VMEM((8, 1024, 128), F32), pltpu.VMEM((8, 1024, 128), BF16)]
        + [pltpu.VMEM((4, 1024, 256), BF16)] * 4,
        compiler_params=params(22),
        name="inverse_root",
    )(idx2, st, *runs, *others)

    other_root = sibling(root)
    back = lax.ppermute(rows, ("co", "pair"), SWAP)
    final = pl.pallas_call(
        update_kernel,
        out_shape=sds((64, 1024), BF16),
        in_specs=[SMEM] + [VMEM] * 4,
        out_specs=VMEM,
        scratch_shapes=[pltpu.VMEM((4, 1024, 256), BF16), pltpu.VMEM((1024, 256), F32), pltpu.VMEM((4, 64, 256), F32)],
        compiler_params=params(16),
        name="update_rows",
    )(idx2, root, other_root, grad, grad_sq)
    update = lax.ppermute(final, ("co", "pair"), SWAP)
    new_rows = 0.9 * stat + back
    return update[None], new_rows[None, None]


def solution(mesh):
    m = Mesh(mesh.devices.reshape(8, 4, 2, 2, 2), ("tok", "y", "xl", "co", "pair"))
    tile = ("y", "xl", "co")
    return jax.shard_map(
        step,
        mesh=m,
        in_specs=(P(("tok", "pair"), tile), P(("tok", "pair"), tile), P(tile, "pair", "tok", None)),
        out_specs=(P(tile, ("tok", "pair"), None), P(tile, "pair", "tok", None)),
        check_vma=False,
    )
```

```python
import jax
import jax.numpy as jnp
from jax import lax
from jax.experimental import pallas as pl
from jax.experimental.pallas import tpu as pltpu
from jax.sharding import Mesh, PartitionSpec as P


F32 = jnp.float32
BF16 = jnp.bfloat16
F16 = jnp.float16
VMEM = pl.BlockSpec(memory_space=pltpu.VMEM)
SMEM = pl.BlockSpec(memory_space=pltpu.SMEM)
Z = 8
SWAP = [(0, 0), (1, 2), (2, 1), (3, 3)]


def params(mib):
    return pltpu.CompilerParams(vmem_limit_bytes=mib * 1024 * 1024)


def sds(shape, dt):
    return jax.ShapeDtypeStruct(shape, dt)


def dot(a, b, ca=1, cb=0):
    return lax.dot_general(a, b, (((ca,), (cb,)), ((), ())), preferred_element_type=F32)


def cat(ref):
    return jnp.concatenate([ref[k] for k in range(ref.shape[0])], axis=1)


def loop(n, body, unroll=1):
    lax.fori_loop(0, n, lambda j, c: (body(j), c)[1], 0, unroll=unroll)


def diagonal(n):
    return lax.broadcasted_iota(jnp.int32, (n, n), 0) == lax.broadcasted_iota(jnp.int32, (n, n), 1)


def partial_kernel(idx, a_own, a_oth, b0, b1, b2, b3, out, acc_s, top):
    co, y = idx[0], idx[2]
    b = (b0, b1, b2, b3)
    top[...] = jnp.zeros(top.shape, F32)
    for h in range(2):
        cb = (y >> 1) ^ h
        for ref, c in ((a_own, co), (a_oth, 1 - co)):
            for l in range(2):
                r = pl.multiple_of(256 * (2 * l + c), 256)
                acc = (dot(ref[2 * l + (y & 1)], b[2 * h][...], 0, 0)
                       + dot(ref[2 * l + 1 - (y & 1)], b[2 * h + 1][...], 0, 0))
                acc_s[cb, pl.ds(r, 256), :] = acc
                top[...] = jnp.maximum(top[...], jnp.max(jnp.abs(acc), axis=0, keepdims=True))
    peak = jnp.max(top[...], axis=1, keepdims=True)
    power = jnp.floor(jnp.log2(jnp.maximum(peak, 1e-30)))
    up = jnp.exp2(14.0 - power)

    def body(k):
        r = pl.multiple_of(128 * k, 128)
        for cb in range(2):
            out[k, :128, 256 * cb:256 * (cb + 1)] = acc_s[cb, pl.ds(r, 128), :] * up
        out[k, 128:, :] = jnp.broadcast_to(power, (8, 512))

    loop(Z, body)


def assemble_kernel(idx, pieces, s_out):
    z = idx[0]
    for d in range(Z):
        rb = (z + Z - d) % Z
        r = pl.multiple_of(rb * 128, 128)
        for k in range(5):
            cb = (rb + k) % Z
            c = pl.multiple_of(cb * 128, 128)
            blk = pieces[d, :, 128 * k:128 * (k + 1)]
            s_out[cb, pl.ds(r, 128), :] = blk
            if 0 < k < 4:
                s_out[rb, pl.ds(c, 128), :] = blk.T


def merge_kernel(idx, mine, theirs, out):
    co = idx[1]
    out[co] = mine[...]
    out[1 - co] = theirs[...]


def half_kernel(idx, src, out):
    out[...] = src[:, pl.ds(pl.multiple_of(64 * idx[1], 64), 64), :]


def chain_kernel(idx, st, g0, r1, r2, r3, r4, o1, o2, o3, o4,
                 root, grad, rows, sq, s_s, x_s, f0, f1, t0, t1):
    z, co = idx[0], idx[1]
    step = 1 - 2 * co
    pieces = [(g0, z, 0), (r1, z - step, 0), (r2, z - 2 * step, 0), (r3, z - 3 * step, 0),
              (o1, z + step, 0), (o2, z + 2 * step, 0), (o3, z + 3 * step, 0),
              (r4, z + 4, 64 * co), (o4, z + 4, 64 * (1 - co))]
    for ref, src, off in pieces:
        n = ref.shape[1]
        blk = (src + 2 * Z) % Z
        r = pl.multiple_of(blk * 128 + off, 64)
        for c in range(2):
            for cb in range(2):
                grad[2 * cb + c, pl.ds(r, n), :] = ref[c, :, 256 * cb:256 * (cb + 1)]

    @pl.when(co == 0)
    def _():
        for j in range(4):
            x_s[2 * j] = grad[j, :, :128]
            x_s[2 * j + 1] = grad[j, :, 128:]

    @pl.when(co == 1)
    def _():
        def body(k):
            r = pl.multiple_of(k * 128, 128)
            for j in range(4):
                x_s[k, 256 * j:256 * (j + 1), :] = grad[j, pl.ds(r, 128), :].T

        loop(Z, body)

    zr = pl.multiple_of(z * 128, 128)

    def product(j, carry):
        top, acc = carry
        r = pl.multiple_of(j * 256, 256)
        p = dot(cat(x_s), jnp.concatenate([x_s[k, pl.ds(r, 256), :] for k in range(Z)], axis=1), 1, 1)
        for h in range(2):
            u = st[2 * j + h] + 0.1 * p[:, 128 * h:128 * (h + 1)]
            s_s[2 * j + h] = u
            top = jnp.maximum(top, jnp.sum(jnp.abs(u), axis=0, keepdims=True))
        v = grad[j].astype(F32)
        return top, acc + jnp.sum(v * v, axis=0, keepdims=True)

    top, acc = lax.fori_loop(0, 4, product, (jnp.zeros((1, 128), F32), jnp.zeros((1, 256), F32)))
    sq[...] = jnp.broadcast_to(jnp.sum(acc, axis=1, keepdims=True), sq.shape)

    for j in range(Z):
        c = slice(128 * j, 128 * (j + 1))
        rows[:, c] = s_s[j, pl.ds(zr, 128), :] - st[j, pl.ds(zr, 128), :]
    bound = jnp.max(top, axis=1, keepdims=True)
    inv = 1.0 / (1.1 * bound)
    ridge = jnp.where(diagonal(128), 0.1 * bound, 0.0)
    five = jnp.where(diagonal(256), 5.0, 0.0)

    def first(j):
        for h in range(2):
            lo = pl.multiple_of(256 * j + 128 * h, 128)
            c = slice(128 * h, 128 * (h + 1))
            t1[j, :, c] = (s_s[2 * j + h] * inv).astype(BF16)
            t1[j, pl.ds(lo, 128), c] = ((s_s[2 * j + h, pl.ds(lo, 128), :] + ridge) * inv).astype(BF16)
        r = pl.multiple_of(256 * j, 256)
        f0[j] = t1[j] * jnp.asarray(-0.25, BF16)
        f0[j, pl.ds(r, 256), :] = ((five - t1[j, pl.ds(r, 256), :].astype(F32)) * 0.25).astype(BF16)

    loop(4, first)

    def mul(dst, a, b):
        def body(j):
            dst[j] = dot(cat(a), b[j]).astype(BF16)

        loop(4, body, 2)

    mul(t0, f0, f0)
    mul(f1, t0, t0)

    def second(j):
        r = pl.multiple_of(256 * j, 256)
        t0[j] = dot(cat(f1), t1[j]).astype(BF16)
        diag = ((five - t0[j, pl.ds(r, 256), :].astype(F32)) * 0.25).astype(BF16)
        t0[j] = t0[j] * jnp.asarray(-0.25, BF16)
        t0[j, pl.ds(r, 256), :] = diag

    loop(4, second)
    mul(root, f0, t0)


def update_kernel(idx, own, other, grad, grad_sq, out, mix, r_s, keep):
    z, co = idx[0], idx[1]
    zr = pl.multiple_of(z * 128 + co * 64, 64)

    def run(left, right):
        def mixed(j):
            mix[j] = dot(cat(left), grad[j]).astype(BF16)

        loop(4, mixed)

        def raw(j, acc):
            r = dot(cat(mix), right[j])
            r_s[...] = r
            keep[j] = r_s[pl.ds(zr, 64), :]
            return acc + jnp.sum(r * r, axis=0, keepdims=True)

        update_sq = jnp.sum(lax.fori_loop(0, 4, raw, jnp.zeros((1, 256), F32)), axis=1, keepdims=True)

        ratio = jnp.sqrt(grad_sq[:1, :1] / (update_sq + 1e-6))
        for j in range(4):
            out[:, 256 * j:256 * (j + 1)] = (keep[j] * ratio).astype(BF16)

    pl.when(co == 0)(lambda: run(own, other))
    pl.when(co == 1)(lambda: run(other, own))


def pack(x, peak):
    power = jnp.floor(jnp.log2(jnp.maximum(peak, 1e-30)))
    scaled = (x * jnp.exp2(14.0 - power)).astype(F16)
    label = jnp.broadcast_to(power, (*x.shape[:-2], 8, x.shape[-1])).astype(F16)
    return jnp.concatenate([scaled, label], axis=-2)


def unpack(x):
    return x[..., :-8, :].astype(F32) * jnp.exp2(x[..., -8:-7, :].astype(F32) - 14.0)


def everyone(x, axis, n):
    return lax.all_to_all(jnp.broadcast_to(x, (n, *x.shape)), axis, 0, 0, tiled=True)


def sibling(x):
    return lax.ppermute(x, "co", [(0, 1), (1, 0)])


def along(x, d):
    return lax.ppermute(x, "tok", [(i, (i + d) % Z) for i in range(Z)])


def step(inputs, output_grads, statistics):
    z = lax.axis_index("tok")
    co = lax.axis_index("co")
    idx1 = jnp.stack([co, z, lax.axis_index("y")]).astype(jnp.int32)
    idx2 = jnp.stack([z, co]).astype(jnp.int32)

    table = [(yy * 4 + xx, xx * 4 + yy) for yy in range(4) for xx in range(4)]
    cot = [lax.ppermute(output_grads, ("y", "xl", "pair"), table)]
    a_own = everyone(inputs, ("xl", "pair"), 4)
    for d in range(1, 4):
        cot.append(lax.ppermute(cot[0], "y", [(i, i ^ d) for i in range(4)]))
    a_oth = sibling(a_own)

    stat = statistics.reshape(128, 1024)
    wide = jnp.concatenate([stat, stat[:, :512]], axis=1)
    part = lax.dynamic_slice(wide, (0, z * 128), (128, 640))
    part = pack(part, jnp.max(jnp.abs(stat)))
    up, down = [part], [part]
    for k in range(1, 5):
        up.append(along(up[-1], 1))
        if k < 4:
            down.append(along(down[-1], -1))

    partial = pl.pallas_call(
        partial_kernel,
        out_shape=sds((Z, 136, 512), F32),
        in_specs=[SMEM] + [VMEM] * 6,
        out_specs=VMEM,
        scratch_shapes=[pltpu.VMEM((2, 1024, 256), F32), pltpu.VMEM((1, 256), F32)],
        compiler_params=params(14),
        name="partial_gradient",
    )(idx1, a_own, a_oth, *cot)

    near = lax.optimization_barrier((partial[0, 128:136, :128], *up[:4], *down[1:]))[1:]
    st = jnp.stack([*near[:4], up[4], *near[:3:-1]])
    st = lax.ppermute(st, ("co", "pair"), SWAP)
    st = pl.pallas_call(
        assemble_kernel,
        out_shape=sds((8, 1024, 128), F32),
        in_specs=[SMEM, VMEM],
        out_specs=VMEM,
        compiler_params=params(10),
        name="assemble",
    )(idx2, 0.9 * unpack(st))

    got = lax.all_to_all(partial.astype(F16), "tok", 0, 0, tiled=True)
    mine = jnp.sum(unpack(got), axis=0).astype(BF16)
    theirs = sibling(mine)
    piece = pl.pallas_call(
        merge_kernel, out_shape=sds((2, 128, 512), BF16), in_specs=[SMEM, VMEM, VMEM], out_specs=VMEM,
        compiler_params=params(2), name="merge",
    )(idx2, mine, theirs)

    def pass_on(x, n):
        perm = []
        for i in range(Z):
            perm += [(2 * i, 2 * ((i + n) % Z)), (2 * i + 1, 2 * ((i - n) % Z) + 1)]
        return lax.ppermute(x, ("tok", "co"), perm)

    two = pass_on(piece, 2)
    one = pass_on(piece, 1)
    half = pl.pallas_call(
        half_kernel, out_shape=sds((2, 64, 512), BF16), in_specs=[SMEM, VMEM], out_specs=VMEM,
        compiler_params=params(2), name="half",
    )(idx2, two)
    runs = [piece, one, two, pass_on(two, 1), pass_on(half, 2)]
    others = [sibling(r) for r in runs[1:]]

    root, grad, rows, grad_sq = pl.pallas_call(
        chain_kernel,
        out_shape=(sds((4, 1024, 256), BF16), sds((4, 1024, 256), BF16), sds((128, 1024), F32), sds((8, 128), F32)),
        in_specs=[SMEM] + [VMEM] * 10,
        out_specs=(VMEM,) * 4,
        scratch_shapes=[pltpu.VMEM((8, 1024, 128), F32), pltpu.VMEM((8, 1024, 128), BF16)]
        + [pltpu.VMEM((4, 1024, 256), BF16)] * 4,
        compiler_params=params(22),
        name="inverse_root",
    )(idx2, st, *runs, *others)

    other_root = sibling(root)
    back = lax.ppermute(rows, ("co", "pair"), SWAP)
    final = pl.pallas_call(
        update_kernel,
        out_shape=sds((64, 1024), BF16),
        in_specs=[SMEM] + [VMEM] * 4,
        out_specs=VMEM,
        scratch_shapes=[pltpu.VMEM((4, 1024, 256), BF16), pltpu.VMEM((1024, 256), F32), pltpu.VMEM((4, 64, 256), F32)],
        compiler_params=params(16),
        name="update_rows",
    )(idx2, root, other_root, grad, grad_sq)
    update = lax.ppermute(final, ("co", "pair"), SWAP)
    new_rows = 0.9 * stat + back
    return update[None], new_rows[None, None]


def solution(mesh):
    m = Mesh(mesh.devices.reshape(8, 4, 2, 2, 2), ("tok", "y", "xl", "co", "pair"))
    tile = ("y", "xl", "co")
    return jax.shard_map(
        step,
        mesh=m,
        in_specs=(P(("tok", "pair"), tile), P(("tok", "pair"), tile), P(tile, "pair", "tok", None)),
        out_specs=(P(tile, ("tok", "pair"), None), P(tile, "pair", "tok", None)),
        check_vma=False,
    )
```

```python
import jax
import jax.numpy as jnp
from jax import lax
from jax.experimental import pallas as pl
from jax.experimental.pallas import tpu as pltpu
from jax.sharding import Mesh, PartitionSpec as P


F32 = jnp.float32
BF16 = jnp.bfloat16
F16 = jnp.float16
VMEM = pl.BlockSpec(memory_space=pltpu.VMEM)
SMEM = pl.BlockSpec(memory_space=pltpu.SMEM)
Z = 8
SWAP = [(0, 0), (1, 2), (2, 1), (3, 3)]


def params(mib):
    return pltpu.CompilerParams(vmem_limit_bytes=mib * 1024 * 1024)


def sds(shape, dt):
    return jax.ShapeDtypeStruct(shape, dt)


def dot(a, b, ca=1, cb=0):
    return lax.dot_general(a, b, (((ca,), (cb,)), ((), ())), preferred_element_type=F32)


def cat(ref):
    return jnp.concatenate([ref[k] for k in range(ref.shape[0])], axis=1)


def loop(n, body, unroll=1):
    lax.fori_loop(0, n, lambda j, c: (body(j), c)[1], 0, unroll=unroll)


def diagonal(n):
    return lax.broadcasted_iota(jnp.int32, (n, n), 0) == lax.broadcasted_iota(jnp.int32, (n, n), 1)


def partial_kernel(idx, a_own, a_oth, b0, b1, b2, b3, out, acc_s, top):
    co, y = idx[0], idx[2]
    b = (b0, b1, b2, b3)
    top[...] = jnp.zeros(top.shape, F32)
    for h in range(2):
        cb = (y >> 1) ^ h
        for ref, c in ((a_own, co), (a_oth, 1 - co)):
            for l in range(2):
                r = pl.multiple_of(256 * (2 * l + c), 256)
                acc = (dot(ref[2 * l + (y & 1)], b[2 * h][...], 0, 0)
                       + dot(ref[2 * l + 1 - (y & 1)], b[2 * h + 1][...], 0, 0))
                acc_s[cb, pl.ds(r, 256), :] = acc
                top[...] = jnp.maximum(top[...], jnp.max(jnp.abs(acc), axis=0, keepdims=True))
    peak = jnp.max(top[...], axis=1, keepdims=True)
    power = jnp.floor(jnp.log2(jnp.maximum(peak, 1e-30)))
    up = jnp.exp2(14.0 - power)

    def body(k):
        r = pl.multiple_of(128 * k, 128)
        for cb in range(2):
            out[k, :128, 256 * cb:256 * (cb + 1)] = acc_s[cb, pl.ds(r, 128), :] * up
        out[k, 128:, :] = jnp.broadcast_to(power, (8, 512))

    loop(Z, body)


def assemble_kernel(idx, pieces, s_out):
    z = idx[0]
    for d in range(Z):
        rb = (z + Z - d) % Z
        r = pl.multiple_of(rb * 128, 128)
        for k in range(5):
            cb = (rb + k) % Z
            c = pl.multiple_of(cb * 128, 128)
            blk = pieces[d, :, 128 * k:128 * (k + 1)]
            s_out[cb, pl.ds(r, 128), :] = blk
            if 0 < k < 4:
                s_out[rb, pl.ds(c, 128), :] = blk.T


def merge_kernel(idx, mine, theirs, out):
    co = idx[1]
    out[co] = mine[...]
    out[1 - co] = theirs[...]


def half_kernel(idx, src, out):
    out[...] = src[:, pl.ds(pl.multiple_of(64 * idx[1], 64), 64), :]


def chain_kernel(idx, st, g0, r1, r2, r3, r4, o1, o2, o3, o4,
                 root, grad, rows, sq, s_s, x_s, f0, f1, t0, t1):
    z, co = idx[0], idx[1]
    step = 1 - 2 * co
    pieces = [(g0, z, 0), (r1, z - step, 0), (r2, z - 2 * step, 0), (r3, z - 3 * step, 0),
              (o1, z + step, 0), (o2, z + 2 * step, 0), (o3, z + 3 * step, 0),
              (r4, z + 4, 64 * co), (o4, z + 4, 64 * (1 - co))]
    for ref, src, off in pieces:
        n = ref.shape[1]
        blk = (src + 2 * Z) % Z
        r = pl.multiple_of(blk * 128 + off, 64)
        for c in range(2):
            for cb in range(2):
                grad[2 * cb + c, pl.ds(r, n), :] = ref[c, :, 256 * cb:256 * (cb + 1)]

    @pl.when(co == 0)
    def _():
        for j in range(4):
            x_s[2 * j] = grad[j, :, :128]
            x_s[2 * j + 1] = grad[j, :, 128:]

    @pl.when(co == 1)
    def _():
        def body(k):
            r = pl.multiple_of(k * 128, 128)
            for j in range(4):
                x_s[k, 256 * j:256 * (j + 1), :] = grad[j, pl.ds(r, 128), :].T

        loop(Z, body)

    zr = pl.multiple_of(z * 128, 128)

    def product(j, carry):
        top, acc = carry
        r = pl.multiple_of(j * 256, 256)
        p = dot(cat(x_s), jnp.concatenate([x_s[k, pl.ds(r, 256), :] for k in range(Z)], axis=1), 1, 1)
        for h in range(2):
            u = st[2 * j + h] + 0.1 * p[:, 128 * h:128 * (h + 1)]
            s_s[2 * j + h] = u
            top = jnp.maximum(top, jnp.sum(jnp.abs(u), axis=0, keepdims=True))
        v = grad[j].astype(F32)
        return top, acc + jnp.sum(v * v, axis=0, keepdims=True)

    top, acc = lax.fori_loop(0, 4, product, (jnp.zeros((1, 128), F32), jnp.zeros((1, 256), F32)), unroll=2)
    sq[...] = jnp.broadcast_to(jnp.sum(acc, axis=1, keepdims=True), sq.shape)

    for j in range(Z):
        c = slice(128 * j, 128 * (j + 1))
        rows[:, c] = s_s[j, pl.ds(zr, 128), :] - st[j, pl.ds(zr, 128), :]
    bound = jnp.max(top, axis=1, keepdims=True)
    inv = 1.0 / (1.1 * bound)
    ridge = jnp.where(diagonal(128), 0.1 * bound, 0.0)
    five = jnp.where(diagonal(256), 5.0, 0.0)

    def first(j):
        for h in range(2):
            lo = pl.multiple_of(256 * j + 128 * h, 128)
            c = slice(128 * h, 128 * (h + 1))
            t1[j, :, c] = (s_s[2 * j + h] * inv).astype(BF16)
            t1[j, pl.ds(lo, 128), c] = ((s_s[2 * j + h, pl.ds(lo, 128), :] + ridge) * inv).astype(BF16)
        r = pl.multiple_of(256 * j, 256)
        f0[j] = t1[j] * jnp.asarray(-0.25, BF16)
        f0[j, pl.ds(r, 256), :] = ((five - t1[j, pl.ds(r, 256), :].astype(F32)) * 0.25).astype(BF16)

    loop(4, first)

    def mul(dst, a, b):
        def body(j):
            dst[j] = dot(cat(a), b[j]).astype(BF16)

        loop(4, body, 4)

    mul(t0, f0, f0)
    mul(f1, t0, t0)

    def second(j):
        r = pl.multiple_of(256 * j, 256)
        t0[j] = dot(cat(f1), t1[j]).astype(BF16)
        diag = ((five - t0[j, pl.ds(r, 256), :].astype(F32)) * 0.25).astype(BF16)
        t0[j] = t0[j] * jnp.asarray(-0.25, BF16)
        t0[j, pl.ds(r, 256), :] = diag

    loop(4, second, 4)
    mul(root, f0, t0)


def update_kernel(idx, own, other, grad, grad_sq, out, mix, r_s, keep):
    z, co = idx[0], idx[1]
    zr = pl.multiple_of(z * 128 + co * 64, 64)

    def run(left, right):
        def mixed(j):
            mix[j] = dot(cat(left), grad[j]).astype(BF16)

        loop(4, mixed, 2)

        def raw(j, acc):
            r = dot(cat(mix), right[j])
            r_s[...] = r
            keep[j] = r_s[pl.ds(zr, 64), :]
            return acc + jnp.sum(r * r, axis=0, keepdims=True)

        update_sq = jnp.sum(lax.fori_loop(0, 4, raw, jnp.zeros((1, 256), F32), unroll=2), axis=1, keepdims=True)

        ratio = jnp.sqrt(grad_sq[:1, :1] / (update_sq + 1e-6))
        for j in range(4):
            out[0, :, 256 * j:256 * (j + 1)] = (keep[j] * ratio).astype(BF16)

    pl.when(co == 0)(lambda: run(own, other))
    pl.when(co == 1)(lambda: run(other, own))


def pack(x, peak):
    power = jnp.floor(jnp.log2(jnp.maximum(peak, 1e-30)))
    scaled = (x * jnp.exp2(14.0 - power)).astype(F16)
    label = jnp.broadcast_to(power, (*x.shape[:-2], 8, x.shape[-1])).astype(F16)
    return jnp.concatenate([scaled, label], axis=-2)


def unpack(x):
    return x[..., :-8, :].astype(F32) * jnp.exp2(x[..., -8:-7, :].astype(F32) - 14.0)


def everyone(x, axis, n):
    return lax.all_to_all(jnp.broadcast_to(x, (n, *x.shape)), axis, 0, 0, tiled=True)


def sibling(x):
    return lax.ppermute(x, "co", [(0, 1), (1, 0)])


def along(x, d):
    return lax.ppermute(x, "tok", [(i, (i + d) % Z) for i in range(Z)])


def step(inputs, output_grads, statistics):
    z = lax.axis_index("tok")
    co = lax.axis_index("co")
    idx1 = jnp.stack([co, z, lax.axis_index("y") ^ lax.axis_index(("xl", "pair"))]).astype(jnp.int32)
    idx2 = jnp.stack([z, co]).astype(jnp.int32)

    table = [(yy * 4 + xx, (xx ^ yy) * 4 + yy) for yy in range(4) for xx in range(4)]
    cot = [lax.ppermute(output_grads, ("y", "xl", "pair"), table)]
    a_own = everyone(inputs, ("xl", "pair"), 4)
    for d in range(1, 4):
        cot.append(lax.ppermute(cot[0], "y", [(i, i ^ d) for i in range(4)]))
    a_oth = sibling(a_own)

    stat = statistics.reshape(128, 1024)
    wide = jnp.concatenate([stat, stat[:, :512]], axis=1)
    part = lax.dynamic_slice(wide, (0, z * 128), (128, 640))
    part = pack(part, jnp.max(jnp.abs(stat)))
    up, down = [part], [part]
    for k in range(1, 5):
        up.append(along(up[-1], 1))
        if k < 4:
            down.append(along(down[-1], -1))

    partial = pl.pallas_call(
        partial_kernel,
        out_shape=sds((Z, 136, 512), F32),
        in_specs=[SMEM] + [VMEM] * 6,
        out_specs=VMEM,
        scratch_shapes=[pltpu.VMEM((2, 1024, 256), F32), pltpu.VMEM((1, 256), F32)],
        compiler_params=params(14),
        name="partial_gradient",
    )(idx1, a_own, a_oth, *cot)

    near = lax.optimization_barrier((partial[0, 128:136, :128], *up[:4], *down[1:]))[1:]
    st = jnp.stack([*near[:4], up[4], *near[:3:-1]])
    st = lax.ppermute(st, ("co", "pair"), SWAP)
    st = pl.pallas_call(
        assemble_kernel,
        out_shape=sds((8, 1024, 128), F32),
        in_specs=[SMEM, VMEM],
        out_specs=VMEM,
        compiler_params=params(10),
        name="assemble",
    )(idx2, 0.9 * unpack(st))

    got = lax.all_to_all(partial.astype(F16), "tok", 0, 0, tiled=True)
    mine = jnp.sum(unpack(got), axis=0).astype(BF16)
    theirs = sibling(mine)
    piece = pl.pallas_call(
        merge_kernel, out_shape=sds((2, 128, 512), BF16), in_specs=[SMEM, VMEM, VMEM], out_specs=VMEM,
        compiler_params=params(2), name="merge",
    )(idx2, mine, theirs)

    def pass_on(x, n):
        perm = []
        for i in range(Z):
            perm += [(2 * i, 2 * ((i + n) % Z)), (2 * i + 1, 2 * ((i - n) % Z) + 1)]
        return lax.ppermute(x, ("tok", "co"), perm)

    two = pass_on(piece, 2)
    one = pass_on(piece, 1)
    half = pl.pallas_call(
        half_kernel, out_shape=sds((2, 64, 512), BF16), in_specs=[SMEM, VMEM], out_specs=VMEM,
        compiler_params=params(2), name="half",
    )(idx2, two)
    runs = [piece, one, two, pass_on(two, 1), pass_on(half, 2)]
    others = [sibling(r) for r in runs[1:]]

    root, grad, rows, grad_sq = pl.pallas_call(
        chain_kernel,
        out_shape=(sds((4, 1024, 256), BF16), sds((4, 1024, 256), BF16), sds((128, 1024), F32), sds((8, 128), F32)),
        in_specs=[SMEM] + [VMEM] * 10,
        out_specs=(VMEM,) * 4,
        scratch_shapes=[pltpu.VMEM((8, 1024, 128), F32), pltpu.VMEM((8, 1024, 128), BF16)]
        + [pltpu.VMEM((4, 1024, 256), BF16)] * 4,
        compiler_params=params(22),
        name="inverse_root",
    )(idx2, st, *runs, *others)

    other_root = sibling(root)
    back = lax.ppermute(rows, ("co", "pair"), SWAP)
    final = pl.pallas_call(
        update_kernel,
        out_shape=sds((1, 64, 1024), BF16),
        in_specs=[SMEM] + [VMEM] * 4,
        out_specs=VMEM,
        scratch_shapes=[pltpu.VMEM((4, 1024, 256), BF16), pltpu.VMEM((1024, 256), F32), pltpu.VMEM((4, 64, 256), F32)],
        compiler_params=params(16),
        name="update_rows",
    )(idx2, root, other_root, grad, grad_sq)
    update = lax.ppermute(final, ("co", "pair"), SWAP)
    new_rows = 0.9 * stat + back
    return update, new_rows[None, None]


def solution(mesh):
    m = Mesh(mesh.devices.reshape(8, 4, 2, 2, 2), ("tok", "y", "xl", "co", "pair"))
    tile = ("y", "xl", "co")
    return jax.shard_map(
        step,
        mesh=m,
        in_specs=(P(("tok", "pair"), tile), P(("tok", "pair"), tile), P(tile, "pair", "tok", None)),
        out_specs=(P(tile, ("tok", "pair"), None), P(tile, "pair", "tok", None)),
        check_vma=False,
    )
```

```python
import jax
import jax.numpy as jnp
from jax import lax
from jax.experimental import pallas as pl
from jax.experimental.pallas import tpu as pltpu
from jax.sharding import Mesh, PartitionSpec as P


F32 = jnp.float32
BF16 = jnp.bfloat16
F16 = jnp.float16
VMEM = pl.BlockSpec(memory_space=pltpu.VMEM)
SMEM = pl.BlockSpec(memory_space=pltpu.SMEM)
Z = 8
SWAP = [(0, 0), (1, 2), (2, 1), (3, 3)]


def params(mib):
    return pltpu.CompilerParams(vmem_limit_bytes=mib * 1024 * 1024)


def sds(shape, dt):
    return jax.ShapeDtypeStruct(shape, dt)


def dot(a, b, ca=1, cb=0):
    return lax.dot_general(a, b, (((ca,), (cb,)), ((), ())), preferred_element_type=F32)


def cat(ref):
    return jnp.concatenate([ref[k] for k in range(ref.shape[0])], axis=1)


def loop(n, body, unroll=1):
    lax.fori_loop(0, n, lambda j, c: (body(j), c)[1], 0, unroll=unroll)


def diagonal(n):
    return lax.broadcasted_iota(jnp.int32, (n, n), 0) == lax.broadcasted_iota(jnp.int32, (n, n), 1)


def partial_kernel(idx, a_own, a_oth, b0, b1, b2, b3, out, acc_s, top):
    co, y = idx[0], idx[2]
    b = (b0, b1, b2, b3)
    top[...] = jnp.zeros(top.shape, F32)
    for h in range(2):
        cb = (y >> 1) ^ h
        for ref, c in ((a_own, co), (a_oth, 1 - co)):
            for l in range(2):
                r = pl.multiple_of(256 * (2 * l + c), 256)
                acc = (dot(ref[2 * l + (y & 1)], b[2 * h][...], 0, 0)
                       + dot(ref[2 * l + 1 - (y & 1)], b[2 * h + 1][...], 0, 0))
                acc_s[cb, pl.ds(r, 256), :] = acc
                top[...] = jnp.maximum(top[...], jnp.max(jnp.abs(acc), axis=0, keepdims=True))
    peak = jnp.max(top[...], axis=1, keepdims=True)
    power = jnp.floor(jnp.log2(jnp.maximum(peak, 1e-30)))
    up = jnp.exp2(14.0 - power)

    def body(k):
        r = pl.multiple_of(128 * k, 128)
        for cb in range(2):
            out[k, :128, 256 * cb:256 * (cb + 1)] = acc_s[cb, pl.ds(r, 128), :] * up
        out[k, 128:, :] = jnp.broadcast_to(power, (8, 512))

    loop(Z, body)


def assemble_kernel(idx, pieces, s_out):
    z = idx[0]
    for d in range(Z):
        rb = (z + Z - d) % Z
        r = pl.multiple_of(rb * 128, 128)
        for k in range(5):
            cb = (rb + k) % Z
            c = pl.multiple_of(cb * 128, 128)
            blk = pieces[d, :, 128 * k:128 * (k + 1)]
            s_out[cb, pl.ds(r, 128), :] = blk
            if 0 < k < 4:
                s_out[rb, pl.ds(c, 128), :] = blk.T


def merge_kernel(idx, mine, theirs, out):
    co = idx[1]
    out[co] = mine[...]
    out[1 - co] = theirs[...]


def half_kernel(idx, src, out):
    out[...] = src[:, pl.ds(pl.multiple_of(64 * idx[1], 64), 64), :]


def chain_kernel(idx, st, g0, r1, r2, r3, r4, o1, o2, o3, o4,
                 root, grad, rows, sq, s_s, x_s, f0, f1, t0, t1):
    z, co = idx[0], idx[1]
    step = 1 - 2 * co
    pieces = [(g0, z, 0), (r1, z - step, 0), (r2, z - 2 * step, 0), (r3, z - 3 * step, 0),
              (o1, z + step, 0), (o2, z + 2 * step, 0), (o3, z + 3 * step, 0),
              (r4, z + 4, 64 * co), (o4, z + 4, 64 * (1 - co))]
    for ref, src, off in pieces:
        n = ref.shape[1]
        blk = (src + 2 * Z) % Z
        r = pl.multiple_of(blk * 128 + off, 64)
        for c in range(2):
            for cb in range(2):
                grad[2 * cb + c, pl.ds(r, n), :] = ref[c, :, 256 * cb:256 * (cb + 1)]

    @pl.when(co == 0)
    def _():
        for j in range(4):
            x_s[2 * j] = grad[j, :, :128]
            x_s[2 * j + 1] = grad[j, :, 128:]

    @pl.when(co == 1)
    def _():
        def body(k):
            r = pl.multiple_of(k * 128, 128)
            for j in range(4):
                x_s[k, 256 * j:256 * (j + 1), :] = grad[j, pl.ds(r, 128), :].T

        loop(Z, body)

    zr = pl.multiple_of(z * 128, 128)

    def product(j, carry):
        top, acc = carry
        r = pl.multiple_of(j * 256, 256)
        p = dot(cat(x_s), jnp.concatenate([x_s[k, pl.ds(r, 256), :] for k in range(Z)], axis=1), 1, 1)
        for h in range(2):
            u = st[2 * j + h] + 0.1 * p[:, 128 * h:128 * (h + 1)]
            s_s[2 * j + h] = u
            top = jnp.maximum(top, jnp.sum(jnp.abs(u), axis=0, keepdims=True))
        v = grad[j].astype(F32)
        return top, acc + jnp.sum(v * v, axis=0, keepdims=True)

    top, acc = lax.fori_loop(0, 4, product, (jnp.zeros((1, 128), F32), jnp.zeros((1, 256), F32)), unroll=4)
    sq[...] = jnp.broadcast_to(jnp.sum(acc, axis=1, keepdims=True), sq.shape)

    for j in range(Z):
        c = slice(128 * j, 128 * (j + 1))
        rows[:, c] = s_s[j, pl.ds(zr, 128), :] - st[j, pl.ds(zr, 128), :]
    bound = jnp.max(top, axis=1, keepdims=True)
    inv = 1.0 / (1.1 * bound)
    ridge = jnp.where(diagonal(128), 0.1 * bound, 0.0)
    five = jnp.where(diagonal(256), 5.0, 0.0)

    def first(j):
        for h in range(2):
            lo = pl.multiple_of(256 * j + 128 * h, 128)
            c = slice(128 * h, 128 * (h + 1))
            t1[j, :, c] = (s_s[2 * j + h] * inv).astype(BF16)
            t1[j, pl.ds(lo, 128), c] = ((s_s[2 * j + h, pl.ds(lo, 128), :] + ridge) * inv).astype(BF16)
        r = pl.multiple_of(256 * j, 256)
        f0[j] = t1[j] * jnp.asarray(-0.25, BF16)
        f0[j, pl.ds(r, 256), :] = ((five - t1[j, pl.ds(r, 256), :].astype(F32)) * 0.25).astype(BF16)

    loop(4, first)

    def mul(dst, a, b):
        def body(j):
            dst[j] = dot(cat(a), b[j]).astype(BF16)

        loop(4, body, 4)

    mul(t0, f0, f0)
    mul(f1, t0, t0)

    def second(j):
        r = pl.multiple_of(256 * j, 256)
        t0[j] = dot(cat(f1), t1[j]).astype(BF16)
        diag = ((five - t0[j, pl.ds(r, 256), :].astype(F32)) * 0.25).astype(BF16)
        t0[j] = t0[j] * jnp.asarray(-0.25, BF16)
        t0[j, pl.ds(r, 256), :] = diag

    loop(4, second, 4)
    mul(root, f0, t0)


def update_kernel(idx, own, other, grad, grad_sq, out, mix, r_s, keep):
    z, co = idx[0], idx[1]
    zr = pl.multiple_of(z * 128 + co * 64, 64)

    def run(left, right):
        def mixed(j):
            mix[j] = dot(cat(left), grad[j]).astype(BF16)

        loop(4, mixed, 4)

        def raw(j, acc):
            r = dot(cat(mix), right[j])
            r_s[...] = r
            keep[j] = r_s[pl.ds(zr, 64), :]
            return acc + jnp.sum(r * r, axis=0, keepdims=True)

        update_sq = jnp.sum(lax.fori_loop(0, 4, raw, jnp.zeros((1, 256), F32), unroll=4), axis=1, keepdims=True)

        ratio = jnp.sqrt(grad_sq[:1, :1] / (update_sq + 1e-6))
        for j in range(4):
            out[0, :, 256 * j:256 * (j + 1)] = (keep[j] * ratio).astype(BF16)

    pl.when(co == 0)(lambda: run(own, other))
    pl.when(co == 1)(lambda: run(other, own))


def pack(x, peak):
    power = jnp.floor(jnp.log2(jnp.maximum(peak, 1e-30)))
    scaled = (x * jnp.exp2(14.0 - power)).astype(F16)
    label = jnp.broadcast_to(power, (*x.shape[:-2], 8, x.shape[-1])).astype(F16)
    return jnp.concatenate([scaled, label], axis=-2)


def unpack(x):
    return x[..., :-8, :].astype(F32) * jnp.exp2(x[..., -8:-7, :].astype(F32) - 14.0)


def everyone(x, axis, n):
    return lax.all_to_all(jnp.broadcast_to(x, (n, *x.shape)), axis, 0, 0, tiled=True)


def sibling(x):
    return lax.ppermute(x, "co", [(0, 1), (1, 0)])


def along(x, d):
    return lax.ppermute(x, "tok", [(i, (i + d) % Z) for i in range(Z)])


def step(inputs, output_grads, statistics):
    z = lax.axis_index("tok")
    co = lax.axis_index("co")
    idx1 = jnp.stack([co, z, lax.axis_index("y")]).astype(jnp.int32)
    idx2 = jnp.stack([z, co]).astype(jnp.int32)

    table = [(yy * 4 + xx, xx * 4 + yy) for yy in range(4) for xx in range(4)]
    cot = [lax.ppermute(output_grads, ("y", "xl", "pair"), table)]
    a_own = everyone(inputs, ("xl", "pair"), 4)
    for d in range(1, 4):
        cot.append(lax.ppermute(cot[0], "y", [(i, i ^ d) for i in range(4)]))
    a_oth = sibling(a_own)

    stat = statistics.reshape(128, 1024)
    wide = jnp.concatenate([stat, stat[:, :512]], axis=1)
    part = lax.dynamic_slice(wide, (0, z * 128), (128, 640))
    part = pack(part, jnp.max(jnp.abs(stat)))
    up, down = [part], [part]
    for k in range(1, 5):
        up.append(along(up[-1], 1))
        if k < 4:
            down.append(along(down[-1], -1))

    partial = pl.pallas_call(
        partial_kernel,
        out_shape=sds((Z, 136, 512), F32),
        in_specs=[SMEM] + [VMEM] * 6,
        out_specs=VMEM,
        scratch_shapes=[pltpu.VMEM((2, 1024, 256), F32), pltpu.VMEM((1, 256), F32)],
        compiler_params=params(14),
        name="partial_gradient",
    )(idx1, a_own, a_oth, *cot)

    near = lax.optimization_barrier((partial[0, 128:136, :128], *up[:4], *down[1:]))[1:]
    st = jnp.stack([*near[:4], up[4], *near[:3:-1]])
    st = lax.ppermute(st, ("co", "pair"), SWAP)
    st = pl.pallas_call(
        assemble_kernel,
        out_shape=sds((8, 1024, 128), F32),
        in_specs=[SMEM, VMEM],
        out_specs=VMEM,
        compiler_params=params(10),
        name="assemble",
    )(idx2, 0.9 * unpack(st))

    got = lax.all_to_all(partial.astype(F16), "tok", 0, 0, tiled=True)
    mine = jnp.sum(unpack(got), axis=0).astype(BF16)
    theirs = sibling(mine)
    piece = pl.pallas_call(
        merge_kernel, out_shape=sds((2, 128, 512), BF16), in_specs=[SMEM, VMEM, VMEM], out_specs=VMEM,
        compiler_params=params(2), name="merge",
    )(idx2, mine, theirs)

    def pass_on(x, n):
        perm = []
        for i in range(Z):
            perm += [(2 * i, 2 * ((i + n) % Z)), (2 * i + 1, 2 * ((i - n) % Z) + 1)]
        return lax.ppermute(x, ("tok", "co"), perm)

    two = pass_on(piece, 2)
    one = pass_on(piece, 1)
    half = pl.pallas_call(
        half_kernel, out_shape=sds((2, 64, 512), BF16), in_specs=[SMEM, VMEM], out_specs=VMEM,
        compiler_params=params(2), name="half",
    )(idx2, two)
    runs = [piece, one, two, pass_on(two, 1), pass_on(half, 2)]
    others = [sibling(r) for r in runs[1:]]

    root, grad, rows, grad_sq = pl.pallas_call(
        chain_kernel,
        out_shape=(sds((4, 1024, 256), BF16), sds((4, 1024, 256), BF16), sds((128, 1024), F32), sds((8, 128), F32)),
        in_specs=[SMEM] + [VMEM] * 10,
        out_specs=(VMEM,) * 4,
        scratch_shapes=[pltpu.VMEM((8, 1024, 128), F32), pltpu.VMEM((8, 1024, 128), BF16)]
        + [pltpu.VMEM((4, 1024, 256), BF16)] * 4,
        compiler_params=params(22),
        name="inverse_root",
    )(idx2, st, *runs, *others)

    other_root = sibling(root)
    back = lax.ppermute(rows, ("co", "pair"), SWAP)
    final = pl.pallas_call(
        update_kernel,
        out_shape=sds((1, 64, 1024), BF16),
        in_specs=[SMEM] + [VMEM] * 4,
        out_specs=VMEM,
        scratch_shapes=[pltpu.VMEM((4, 1024, 256), BF16), pltpu.VMEM((1024, 256), F32), pltpu.VMEM((4, 64, 256), F32)],
        compiler_params=params(16),
        name="update_rows",
    )(idx2, root, other_root, grad, grad_sq)
    update = lax.ppermute(final, ("co", "pair"), SWAP)
    new_rows = 0.9 * stat + back
    return update, new_rows[None, None]


def solution(mesh):
    m = Mesh(mesh.devices.reshape(8, 4, 2, 2, 2), ("tok", "y", "xl", "co", "pair"))
    tile = ("y", "xl", "co")
    return jax.shard_map(
        step,
        mesh=m,
        in_specs=(P(("tok", "pair"), tile), P(("tok", "pair"), tile), P(tile, "pair", "tok", None)),
        out_specs=(P(tile, ("tok", "pair"), None), P(tile, "pair", "tok", None)),
        check_vma=False,
    )
```
